16 devices in a mesh: rep: 2 (over y, z), dp: 8 (over x, core).
Axes of the slice: x: 4, y: 2, z: 1, core: 2. Of those that a mesh axis runs over, the one named last changes fastest.
The devices are a block of a 4x4x8 slice.
Arguments:
- g_w_gate: bfloat16 [16, 2, 1024, 3200], P(('rep', 'dp')), parts along dimension 0
- g_w_up: bfloat16 [16, 2, 1024, 3200], P(('rep', 'dp')), parts along dimension 0
- g_w_down: bfloat16 [16, 2, 3200, 1024], P(('rep', 'dp')), parts along dimension 0
- w_gate: bfloat16 [2, 1024, 3200], replicated
- w_up: bfloat16 [2, 1024, 3200], replicated
- w_down: bfloat16 [2, 3200, 1024], replicated
- m_w_gate: float32 [2, 1024, 3200], P(None, 'dp')
- m_w_up: float32 [2, 1024, 3200], P(None, 'dp')
- m_w_down: float32 [2, 3200, 1024], P(None, 'dp')
- v_w_gate: float32 [2, 1024, 3200], P(None, 'dp')
- v_w_up: float32 [2, 1024, 3200], P(None, 'dp')
- v_w_down: float32 [2, 3200, 1024], P(None, 'dp')
Outputs:
- output 1: bfloat16 [4, 1024, 3200], P('rep'), parts along dimension 0
- output 2: bfloat16 [4, 1024, 3200], P('rep'), parts along dimension 0
- output 3: bfloat16 [4, 3200, 1024], P('rep'), parts along dimension 0
- output 4: float32 [4, 1024, 3200], P('rep', 'dp'), parts along dimension 0
- output 5: float32 [4, 1024, 3200], P('rep', 'dp'), parts along dimension 0
- output 6: float32 [4, 3200, 1024], P('rep', 'dp'), parts along dimension 0
- output 7: float32 [4, 1024, 3200], P('rep', 'dp'), parts along dimension 0
- output 8: float32 [4, 1024, 3200], P('rep', 'dp'), parts along dimension 0
- output 9: float32 [4, 3200, 1024], P('rep', 'dp'), parts along dimension 0
There are 2 independent parts. The reference program is written for one: setup_inputs(seed, part) draws one part's arguments, and reference() takes and returns one part's arrays. A program takes and returns all parts, laid end to end along the dimension named above; an argument that names none is the same for every part.
All inputs are finite; a program needn't handle non-finite values.
Results may differ from the reference program's by a relative error of at most 0.022.
Values are sent between devices in bfloat16 or wider.
A program may use at most 768 MiB of HBM per device.

```python
import jax
import jax.numpy as jnp
from jax import lax

DEVICES = 8
D = 1024
FF = 3200
LAYERS = 2
NAMES = ("w_gate", "w_up", "w_down")
SHAPES = {"w_gate": (LAYERS, D, FF), "w_up": (LAYERS, D, FF), "w_down": (LAYERS, FF, D)}


def setup_inputs(seed: int = 0, part: int = 0) -> dict:
    kz, *keys = jax.random.split(jax.random.key(seed), 1 + 5 * len(NAMES))
    loud = 2.0 ** jax.random.uniform(kz, (), jnp.float32, -1.0, 1.0)
    drawn = {}
    for name, key, both in zip(NAMES, keys[:3], keys[3:6], strict=True):
        own = jax.random.normal(jax.random.fold_in(key, part), (DEVICES, *SHAPES[name]), jnp.float32)
        shared = jax.random.normal(jax.random.fold_in(both, part), SHAPES[name], jnp.float32)
        drawn["g_" + name] = (loud * (0.7 * shared / DEVICES + 0.7 * own * DEVICES**-0.5)).astype(jnp.bfloat16)
    for name, key in zip(NAMES, keys[6:9], strict=True):
        drawn[name] = (jax.random.normal(key, SHAPES[name], jnp.float32) * SHAPES[name][1] ** -0.5).astype(jnp.bfloat16)
    for name, key in zip(NAMES, keys[9:12], strict=True):
        drawn["m_" + name] = loud * 0.5 * jax.random.normal(key, SHAPES[name], jnp.float32)
    for name, key in zip(NAMES, keys[12:15], strict=True):
        drawn["v_" + name] = loud * loud * jax.random.uniform(key, SHAPES[name], jnp.float32, 0.5, 1.5)
    return drawn


def adamw(w, m, v, g):
    m = 0.9 * m + 0.1 * g
    v = 0.95 * v + 0.05 * g * g
    step = m * lax.rsqrt(v + 1e-8) + 0.1 * w
    return (w - 0.02 * step).astype(jnp.bfloat16), m, v


def reference(g_w_gate, g_w_up, g_w_down, w_gate, w_up, w_down, m_w_gate, m_w_up, m_w_down, v_w_gate, v_w_up, v_w_down):
    def total(terms):
        return lax.scan(lambda so_far, term: (so_far + term.astype(jnp.float32), None), jnp.zeros(terms.shape[1:], jnp.float32), terms)[0]

    gradients = [total(terms).astype(jnp.bfloat16).astype(jnp.float32) for terms in (g_w_gate, g_w_up, g_w_down)]
    new = [
        adamw(w.astype(jnp.float32), m, v, g)
        for w, m, v, g in zip((w_gate, w_up, w_down), (m_w_gate, m_w_up, m_w_down), (v_w_gate, v_w_up, v_w_down), gradients, strict=True)
    ]
    return tuple(one[which] for which in range(3) for one in new)
```

```python
import functools

import jax
import jax.numpy as jnp
from jax import lax
from jax.experimental import pallas as pl
from jax.experimental.pallas import tpu as pltpu
from jax.sharding import PartitionSpec as P

MESH = pl.DeviceIdType.MESH
F32, BF16 = jnp.float32, jnp.bfloat16
CHIPS = 4
OPPOSITE, RIGHT, LEFT, OWN = range(4)
OFFSET = (2, 1, 3, 0)


def adamw(w, m, v, g):
    m = 0.9 * m + 0.1 * g
    v = 0.95 * v + 0.05 * g * g
    step = m * lax.rsqrt(v + 1e-8) + 0.1 * w
    return (w - 0.02 * step).astype(BF16), m, v


def rows_16(rows, cols, width, body):
    start, stop = rows

    @pl.loop(0, (stop - start) // 16)
    def _(t):
        r = pl.ds(pl.multiple_of(start + t * 16, 16), 16)
        for c in range(0, cols, width):
            body(r, pl.ds(c, width))


class Chunk:
    def __init__(self, number, which, layer, kind, place, block):
        self.number, self.which, self.layer = number, which, layer
        self.kind, self.place = kind, place
        self.block, self.cols = block
        half = self.block // 32 * 16
        if self.block - half != half and layer % 2 == 0:
            half = self.block - half
        self.half = half
        self.width = 640 if self.cols % 640 == 0 else 512

    def rows(self, part):
        return {"a": (0, self.half), "b": (self.half, self.block), "ab": (0, self.block)}[part]


def chunks_of(shapes):
    kinds, chunks, used = [], [], []
    for which, (layers, rows, cols) in enumerate(shapes):
        block = (rows // (2 * CHIPS), cols)
        if block not in kinds:
            kinds.append(block)
            used.append(0)
        kind = kinds.index(block)
        for layer in range(layers):
            chunks.append(Chunk(len(chunks), which, layer, kind, used[kind], block))
            used[kind] += 1
    return chunks, kinds, used


def exchange(chunks, kinds, tail, *refs):
    it = iter(refs)
    take = lambda n: [next(it) for _ in range(n)]
    g, w, m, v = take(3), take(3), take(3), take(3)
    out, new_m, new_v = take(3), take(3), take(3)
    nk = len(kinds)
    peer, pass_in, near_in, own, w_in, m_in, v_in = (take(nk) for _ in range(7))
    (x_send, x_recv, a_send, a_recv, b_send, b_recv, own_sem, in_sem, out_sem,
     g1_send, g1_recv, g2_send, g2_recv, gx_send, gx_recv) = it
    n = len(chunks)

    me = lax.axis_index("dp")
    chip, core = me // 2, me % 2
    right = lax.rem(chip + 1, CHIPS) * 2 + core
    left = lax.rem(chip + CHIPS - 1, CHIPS) * 2 + core
    other = chip * 2 + (1 - core)
    chip_at = [lax.rem(chip + OFFSET[r], CHIPS) for r in range(4)]

    barrier = pltpu.get_barrier_semaphore()
    for d in (right, left, other):
        pl.semaphore_signal(barrier, inc=1, device_id={"dp": d}, device_id_type=MESH)

    pending = []

    def remote(src, dst, send, recv, to):
        copy = pltpu.make_async_remote_copy(
            src_ref=src, dst_ref=dst, send_sem=send, recv_sem=recv, device_id={"dp": to}, device_id_type=MESH)
        copy.start()
        pending.append(copy)
        return copy

    def block_rows(c, block, part="ab"):
        start, stop = c.rows(part)
        return pl.ds(pl.multiple_of(block * c.block + start, 16), stop - start)

    order = [(OPPOSITE, c) for c in chunks]
    for c in chunks:
        order += [(RIGHT, c), (LEFT, c)]
    order += [(OWN, c) for c in chunks]
    slots, seen = {}, [0] * nk
    for r, c in order:
        slots[r, c.number] = seen[c.kind] % 3
        seen[c.kind] += 1

    def own_load(p):
        r, c = order[p]
        return pltpu.make_async_copy(
            g[c.which].at[c.layer, block_rows(c, chip_at[r] * 2 + core), :],
            own[c.kind].at[slots[r, c.number]], own_sem.at[r * n + c.number])

    def state_loads(c):
        s = c.place % 2
        return [
            pltpu.make_async_copy(w[c.which].at[c.layer, block_rows(c, me), :], w_in[c.kind].at[s], in_sem.at[c.number * 3]),
            pltpu.make_async_copy(m[c.which].at[c.layer], m_in[c.kind].at[s], in_sem.at[c.number * 3 + 1]),
            pltpu.make_async_copy(v[c.which].at[c.layer], v_in[c.kind].at[s], in_sem.at[c.number * 3 + 2]),
        ]

    own_load(0).start()
    own_load(1).start()
    pl.semaphore_wait(barrier, 3)

    x = {}

    def swap(r, c):
        x[r, c.number] = remote(
            g[c.which].at[c.layer, block_rows(c, chip_at[r] * 2 + (1 - core)), :], peer[c.kind].at[r, c.place],
            x_send.at[r * n + c.number], x_recv.at[r * n + c.number], other)

    for c in chunks:
        swap(OPPOSITE, c)

    position = [0]

    def take_own(r, c):
        p = position[0]
        position[0] += 1
        assert order[p] == (r, c)
        if p + 2 < len(order):
            own_load(p + 2).start()
        own_load(p).wait()
        x[r, c.number].wait_recv()
        return own[c.kind].at[slots[r, c.number]], peer[c.kind].at[r, c.place]

    def add(c, part, mine, theirs, *more):
        def tile(rows, cols):
            total = mine[rows, cols].astype(F32) + theirs[rows, cols].astype(F32)
            for ref in more:
                total += ref[rows, cols].astype(F32)
            theirs[rows, cols] = total.astype(BF16)

        rows_16(c.rows(part), c.cols, c.width, tile)

    def part_of(ref, c, part):
        start, stop = c.rows(part)
        return ref.at[pl.ds(start, stop - start), :]

    step0 = {}
    for c in chunks:
        mine, theirs = take_own(OPPOSITE, c)
        for part, to, side in (("a", right, 0), ("b", left, 1)):
            add(c, part, mine, theirs)
            step0[side, c.number] = remote(
                part_of(theirs, c, part), part_of(pass_in[c.kind].at[c.place], c, part),
                a_send.at[side * n + c.number], a_recv.at[side * n + c.number], to)
        swap(RIGHT, c)
        swap(LEFT, c)

    step1 = {}
    for c in chunks:
        for r, to, side, parts in ((RIGHT, right, 0, "ab"), (LEFT, left, 1, "ba")):
            mine, theirs = take_own(r, c)
            for k, part in enumerate(parts):
                if k == 0:
                    step0[side, c.number].wait_recv()
                    add(c, part, mine, theirs, pass_in[c.kind].at[c.place])
                else:
                    add(c, part, mine, theirs)
                s = (side * n + c.number) * 2 + k
                step1[side, c.number, k] = remote(
                    part_of(theirs, c, part), part_of(near_in[c.kind].at[side, c.place], c, part),
                    b_send.at[s], b_recv.at[s], to)
        swap(OWN, c)

    for c in chunks[:2]:
        for copy in state_loads(c):
            copy.start()
    hop1, crossing, stores = {}, [], {}

    def cross(ref_rows, c, s):
        crossing.append(remote(
            out[c.which].at[c.layer, ref_rows, :], out[c.which].at[c.layer, ref_rows, :], gx_send.at[s], gx_recv.at[s], other))

    for c in chunks:
        mine, theirs = take_own(OWN, c)
        for copy in state_loads(c):
            copy.wait()
        for side in (0, 1):
            for k in (0, 1):
                step1[side, c.number, k].wait_recv()
        s = c.place % 2
        from_left, from_right = near_in[c.kind].at[0, c.place], near_in[c.kind].at[1, c.place]
        w_ref, m_ref, v_ref = w_in[c.kind].at[s], m_in[c.kind].at[s], v_in[c.kind].at[s]

        def tile(rows, cols):
            total = mine[rows, cols].astype(F32) + theirs[rows, cols].astype(F32)
            total += from_left[rows, cols].astype(F32) + from_right[rows, cols].astype(F32)
            gradient = total.astype(BF16).astype(F32)
            new = adamw(w_ref[rows, cols].astype(F32), m_ref[rows, cols], v_ref[rows, cols], gradient)
            theirs[rows, cols], m_ref[rows, cols], v_ref[rows, cols] = new

        rows_16(c.rows("ab"), c.cols, c.width, tile)
        rows = block_rows(c, me)
        target = out[c.which].at[c.layer, rows, :]
        for side, to in ((0, right), (1, left)):
            hop1[side, c.number] = remote(theirs, target, g1_send.at[side * n + c.number], g1_recv.at[side * n + c.number], to)
        crossing.append(remote(theirs, target, gx_send.at[c.number], gx_recv.at[c.number], other))
        stores[c.number] = [
            pltpu.make_async_copy(theirs, target, out_sem.at[c.number * 3]),
            pltpu.make_async_copy(m_ref, new_m[c.which].at[c.layer], out_sem.at[c.number * 3 + 1]),
            pltpu.make_async_copy(v_ref, new_v[c.which].at[c.layer], out_sem.at[c.number * 3 + 2]),
        ]
        for copy in stores[c.number]:
            copy.start()
        if c.number + 1 < n and c.number >= 1:
            following = chunks[c.number + 1]
            for before in chunks[:c.number]:
                if before.kind == following.kind and before.place == following.place - 2:
                    for copy in stores.pop(before.number):
                        copy.wait()
            for copy in state_loads(following):
                copy.start()

    hop2 = {}
    for c in chunks:
        for side, source, to, part in ((0, LEFT, right, "a"), (1, RIGHT, left, "b")):
            s = side * n + c.number
            hop1[side, c.number].wait_recv()
            block = chip_at[source] * 2 + core
            if c.number not in tail:
                rows = block_rows(c, block, part)
                ref = out[c.which].at[c.layer, rows, :]
                hop2[side, c.number] = remote(ref, ref, g2_send.at[s], g2_recv.at[s], to)
            cross(block_rows(c, block), c, n + s)
    for c in chunks:
        if c.number in tail:
            continue
        for side, part in ((0, "a"), (1, "b")):
            s = side * n + c.number
            hop2[side, c.number].wait_recv()
            cross(block_rows(c, chip_at[OPPOSITE] * 2 + core, part), c, 3 * n + s)
    for copy in crossing:
        copy.wait_recv()
    for copies in stores.values():
        for copy in copies:
            copy.wait()
    for copy in pending:
        copy.wait_send()


def gather_step(tail, terms, weights, m, v):
    shapes = [w.shape for w in weights]
    chunks, kinds, used = chunks_of(shapes)
    n = len(chunks)
    hbm = pl.BlockSpec(memory_space=pl.ANY)
    slots = lambda lead, dtype: [pltpu.VMEM((*(u if x is None else x for x in lead), *k), dtype) for k, u in zip(kinds, used)]
    dma = lambda count: pltpu.SemaphoreType.DMA((count,))
    return pl.pallas_call(
        functools.partial(exchange, chunks, kinds, tail),
        out_shape=[jax.ShapeDtypeStruct(s, BF16) for s in shapes] + [jax.ShapeDtypeStruct(a.shape, F32) for a in (*m, *v)],
        in_specs=[hbm] * 12,
        out_specs=[hbm] * 9,
        scratch_shapes=[
            *slots((4, None), BF16), *slots((None,), BF16), *slots((2, None), BF16), *slots((3,), BF16),
            *slots((2,), BF16), *slots((2,), F32), *slots((2,), F32),
            dma(4 * n), dma(4 * n), dma(2 * n), dma(2 * n), dma(4 * n), dma(4 * n), dma(4 * n), dma(3 * n), dma(3 * n),
            dma(2 * n), dma(2 * n), dma(2 * n), dma(2 * n), dma(5 * n), dma(5 * n),
        ],
        compiler_params=pltpu.CompilerParams(collective_id=0, has_side_effects=True, vmem_limit_bytes=63 * 2**20),
    )(*terms, *weights, *m, *v)


def solution(mesh):
    assert mesh.shape["dp"] == 2 * CHIPS

    def step(*arrays):
        terms, weights, m, v = (arrays[i : i + 3] for i in (0, 3, 6, 9))
        return tuple(gather_step((), [t[0] for t in terms], weights, m, v))

    all_of, cut = P(None, None, None), P(None, "dp", None)
    return jax.shard_map(
        step,
        mesh=mesh,
        in_specs=(P(("rep", "dp"), None, None, None),) * 3 + (all_of,) * 3 + (cut,) * 6,
        out_specs=(P("rep", None, None),) * 3 + (P("rep", "dp", None),) * 6,
        check_vma=False,
    )
```

```python
import functools

import jax
import jax.numpy as jnp
from jax import lax
from jax.experimental import pallas as pl
from jax.experimental.pallas import tpu as pltpu
from jax.sharding import PartitionSpec as P


MESH = pl.DeviceIdType.MESH
F32, BF16 = jnp.float32, jnp.bfloat16
CHIPS = 4
OPPOSITE, RIGHT, LEFT, OWN = range(4)
OFFSET = (2, 1, 3, 0)


def adamw(w, m, v, g):
    m = 0.9 * m + 0.1 * g
    v = 0.95 * v + 0.05 * g * g
    step = m * lax.rsqrt(v + 1e-8) + 0.1 * w
    return (w - 0.02 * step).astype(BF16), m, v


def rows_16(rows, cols, width, body):
    start, stop = rows

    @pl.loop(0, (stop - start) // 16)
    def _(t):
        r = pl.ds(pl.multiple_of(start + t * 16, 16), 16)
        for c in range(0, cols, width):
            body(r, pl.ds(c, width))


class Chunk:
    def __init__(self, number, which, layer, kind, place, block):
        self.number, self.which, self.layer = number, which, layer
        self.kind, self.place = kind, place
        self.block, self.cols = block
        half = self.block // 32 * 16
        if self.block - half != half and layer % 2 == 0:
            half = self.block - half
        self.half = half
        self.width = 640 if self.cols % 640 == 0 else 512

    def rows(self, part):
        return {"a": (0, self.half), "b": (self.half, self.block), "ab": (0, self.block)}[part]


def chunks_of(shapes):
    kinds, chunks, used = [], [], []
    for which, (layers, rows, cols) in enumerate(shapes):
        block = (rows // (2 * CHIPS), cols)
        if block not in kinds:
            kinds.append(block)
            used.append(0)
        kind = kinds.index(block)
        for layer in range(layers):
            chunks.append(Chunk(len(chunks), which, layer, kind, used[kind], block))
            used[kind] += 1
    return chunks, kinds, used


def exchange(chunks, kinds, stages, *refs):
    it = iter(refs)
    take = lambda n: [next(it) for _ in range(n)]
    g, w, m, v = take(3), take(3), take(3), take(3)
    out, new_m, new_v = take(3), take(3), take(3)
    for_right, for_left = take(len(stages)), take(len(stages))
    nk = len(kinds)
    peer, pass_in, near_in, own, w_in, m_in, v_in = (take(nk) for _ in range(7))
    (x_send, x_recv, a_send, a_recv, b_send, b_recv, own_sem, in_sem, out_sem,
     g_send, g_recv, gx_send, gx_recv) = it
    n = len(chunks)

    me = lax.axis_index("dp")
    chip, core = me // 2, me % 2
    right = lax.rem(chip + 1, CHIPS) * 2 + core
    left = lax.rem(chip + CHIPS - 1, CHIPS) * 2 + core
    other = chip * 2 + (1 - core)
    chip_at = [lax.rem(chip + OFFSET[r], CHIPS) for r in range(4)]

    barrier = pltpu.get_barrier_semaphore()
    for d in (right, left, other):
        pl.semaphore_signal(barrier, inc=1, device_id={"dp": d}, device_id_type=MESH)

    pending = []

    def remote(src, dst, send, recv, to):
        copy = pltpu.make_async_remote_copy(
            src_ref=src, dst_ref=dst, send_sem=send, recv_sem=recv, device_id={"dp": to}, device_id_type=MESH)
        copy.start()
        pending.append(copy)
        return copy

    def block_rows(c, block, part="ab"):
        start, stop = c.rows(part)
        return pl.ds(pl.multiple_of(block * c.block + start, 16), stop - start)

    order = [(OPPOSITE, c) for c in chunks]
    for c in chunks:
        order += [(RIGHT, c), (LEFT, c)]
    order += [(OWN, c) for c in chunks]
    slots, seen = {}, [0] * nk
    for r, c in order:
        slots[r, c.number] = seen[c.kind] % 3
        seen[c.kind] += 1

    def own_load(p):
        r, c = order[p]
        return pltpu.make_async_copy(
            g[c.which].at[c.layer, block_rows(c, chip_at[r] * 2 + core), :],
            own[c.kind].at[slots[r, c.number]], own_sem.at[r * n + c.number])

    def state_loads(c):
        s = c.place % 2
        return [
            pltpu.make_async_copy(w[c.which].at[c.layer, block_rows(c, me), :], w_in[c.kind].at[s], in_sem.at[c.number * 3]),
            pltpu.make_async_copy(m[c.which].at[c.layer], m_in[c.kind].at[s], in_sem.at[c.number * 3 + 1]),
            pltpu.make_async_copy(v[c.which].at[c.layer], v_in[c.kind].at[s], in_sem.at[c.number * 3 + 2]),
        ]

    own_load(0).start()
    own_load(1).start()
    pl.semaphore_wait(barrier, 3)

    x = {}

    def swap(r, c):
        x[r, c.number] = remote(
            g[c.which].at[c.layer, block_rows(c, chip_at[r] * 2 + (1 - core)), :], peer[c.kind].at[r, c.place],
            x_send.at[r * n + c.number], x_recv.at[r * n + c.number], other)

    for c in chunks:
        swap(OPPOSITE, c)

    position = [0]

    def take_own(r, c):
        p = position[0]
        position[0] += 1
        assert order[p] == (r, c)
        if p + 2 < len(order):
            own_load(p + 2).start()
        own_load(p).wait()
        x[r, c.number].wait_recv()
        return own[c.kind].at[slots[r, c.number]], peer[c.kind].at[r, c.place]

    def add(c, part, mine, theirs, *more):
        def tile(rows, cols):
            total = mine[rows, cols].astype(F32) + theirs[rows, cols].astype(F32)
            for ref in more:
                total += ref[rows, cols].astype(F32)
            theirs[rows, cols] = total.astype(BF16)

        rows_16(c.rows(part), c.cols, c.width, tile)

    def part_of(ref, c, part):
        start, stop = c.rows(part)
        return ref.at[pl.ds(start, stop - start), :]

    step0 = {}
    for c in chunks:
        mine, theirs = take_own(OPPOSITE, c)
        for part, to, side in (("a", right, 0), ("b", left, 1)):
            add(c, part, mine, theirs)
            step0[side, c.number] = remote(
                part_of(theirs, c, part), part_of(pass_in[c.kind].at[c.place], c, part),
                a_send.at[side * n + c.number], a_recv.at[side * n + c.number], to)
        swap(RIGHT, c)
        swap(LEFT, c)

    step1 = {}
    for c in chunks:
        for r, to, side, parts in ((RIGHT, right, 0, "ab"), (LEFT, left, 1, "ba")):
            mine, theirs = take_own(r, c)
            for k, part in enumerate(parts):
                if k == 0:
                    step0[side, c.number].wait_recv()
                    add(c, part, mine, theirs, pass_in[c.kind].at[c.place])
                else:
                    add(c, part, mine, theirs)
                s = (side * n + c.number) * 2 + k
                step1[side, c.number, k] = remote(
                    part_of(theirs, c, part), part_of(near_in[c.kind].at[side, c.place], c, part),
                    b_send.at[s], b_recv.at[s], to)
        swap(OWN, c)

    for c in chunks[:2]:
        for copy in state_loads(c):
            copy.start()
    arrivals, crossing, stores = {}, [], {}

    def passed_on(c, part):
        stage, layer = c.stage
        return (for_right if part == "a" else for_left)[stage].at[layer]

    def kept(c, block, part="ab"):
        return out[c.which].at[c.layer, block_rows(c, block, part), :]

    for c in chunks:
        mine, theirs = take_own(OWN, c)
        for copy in state_loads(c):
            copy.wait()
        for side in (0, 1):
            for k in (0, 1):
                step1[side, c.number, k].wait_recv()
        s = c.place % 2
        from_left, from_right = near_in[c.kind].at[0, c.place], near_in[c.kind].at[1, c.place]
        w_ref, m_ref, v_ref = w_in[c.kind].at[s], m_in[c.kind].at[s], v_in[c.kind].at[s]

        def tile(rows, cols):
            total = mine[rows, cols].astype(F32) + theirs[rows, cols].astype(F32)
            total += from_left[rows, cols].astype(F32) + from_right[rows, cols].astype(F32)
            gradient = total.astype(BF16).astype(F32)
            new = adamw(w_ref[rows, cols].astype(F32), m_ref[rows, cols], v_ref[rows, cols], gradient)
            theirs[rows, cols], m_ref[rows, cols], v_ref[rows, cols] = new

        rows_16(c.rows("ab"), c.cols, c.width, tile)
        target = kept(c, me)
        for side, to in ((0, right), (1, left)):
            for k, part in enumerate("ab"):
                s = (side * n + c.number) * 2 + k
                arrivals[side, c.number, k] = remote(
                    part_of(theirs, c, part), passed_on(c, part) if side == k else kept(c, me, part),
                    g_send.at[s], g_recv.at[s], to)
        crossing.append(remote(theirs, target, gx_send.at[c.number], gx_recv.at[c.number], other))
        stores[c.number] = [
            pltpu.make_async_copy(theirs, target, out_sem.at[c.number * 3]),
            pltpu.make_async_copy(m_ref, new_m[c.which].at[c.layer], out_sem.at[c.number * 3 + 1]),
            pltpu.make_async_copy(v_ref, new_v[c.which].at[c.layer], out_sem.at[c.number * 3 + 2]),
        ]
        for copy in stores[c.number]:
            copy.start()
        if c.number + 1 < n and c.number >= 1:
            following = chunks[c.number + 1]
            for before in chunks[:c.number]:
                if before.kind == following.kind and before.place == following.place - 2:
                    for copy in stores.pop(before.number):
                        copy.wait()
            for copy in state_loads(following):
                copy.start()

    for c in chunks:
        for k, part in enumerate("ab"):
            for side, source in ((0, LEFT), (1, RIGHT)):
                s = (side * n + c.number) * 2 + k
                arrivals[side, c.number, k].wait_recv()
                there = kept(c, chip_at[source] * 2 + core, part)
                crossing.append(remote(
                    passed_on(c, part) if side == k else there, there, gx_send.at[n + s], gx_recv.at[n + s], other))
    for copy in crossing:
        copy.wait_recv()
    for copies in stores.values():
        for copy in copies:
            copy.wait()
    for copy in pending:
        copy.wait_send()


def gather_step(chunks, kinds, used, stages, terms, weights, m, v):
    n = len(chunks)
    hbm = pl.BlockSpec(memory_space=pl.ANY)
    slots = lambda lead, dtype: [pltpu.VMEM((*(u if x is None else x for x in lead), *k), dtype) for k, u in zip(kinds, used)]
    dma = lambda count: pltpu.SemaphoreType.DMA((count,))
    part = lambda stage, part: jax.ShapeDtypeStruct(
        (len(stage), stage[0].rows(part)[1] - stage[0].rows(part)[0], stage[0].cols), BF16)
    results = [jax.ShapeDtypeStruct(w.shape, BF16) for w in weights]
    results += [jax.ShapeDtypeStruct(a.shape, F32) for a in (*m, *v)]
    results += [part(s, "a") for s in stages] + [part(s, "b") for s in stages]
    return pl.pallas_call(
        functools.partial(exchange, chunks, kinds, stages),
        out_shape=results,
        in_specs=[hbm] * 12,
        out_specs=[hbm] * len(results),
        scratch_shapes=[
            *slots((4, None), BF16), *slots((None,), BF16), *slots((2, None), BF16), *slots((3,), BF16),
            *slots((2,), BF16), *slots((2,), F32), *slots((2,), F32),
            dma(4 * n), dma(4 * n), dma(2 * n), dma(2 * n), dma(4 * n), dma(4 * n), dma(4 * n), dma(3 * n), dma(3 * n),
            dma(4 * n), dma(4 * n), dma(5 * n), dma(5 * n),
        ],
        compiler_params=pltpu.CompilerParams(collective_id=0, has_side_effects=True, vmem_limit_bytes=63 * 2**20),
    )(*terms, *weights, *m, *v)


class Move:
    def __init__(self, source, source_at, target, target_at, rows):
        self.source, self.source_at = source, source_at
        self.target, self.target_at = target, target_at
        self.rows = rows


def move_body(moves, kinds, depth, n_in, n_out, *refs):
    sources, targets = refs[:n_in], refs[n_in : n_in + n_out]
    bufs, (in_sem, out_sem) = refs[n_in + n_out : -2], refs[-2:]
    me = lax.axis_index("dp")
    chip, core = me // 2, me % 2
    seen, place = [0] * len(kinds), []
    for u in moves:
        place.append((u.kind, seen[u.kind] % depth[u.kind]))
        seen[u.kind] += 1

    def view(ref, at, rows):
        layer, row = at(chip, core)
        return ref.at[layer, pl.ds(row if isinstance(row, int) else pl.multiple_of(row, 8), rows), :]

    def load(i):
        u, (kind, slot) = moves[i], place[i]
        return pltpu.make_async_copy(view(sources[u.source], u.source_at, u.rows), bufs[kind].at[slot], in_sem.at[i])

    def store(i):
        u, (kind, slot) = moves[i], place[i]
        return pltpu.make_async_copy(bufs[kind].at[slot], view(targets[u.target], u.target_at, u.rows), out_sem.at[i])

    waited, last = set(), {}

    def start(i):
        if place[i] in last:
            store(last[place[i]]).wait()
            waited.add(last[place[i]])
        last[place[i]] = i
        load(i).start()

    ahead = 8
    for i in range(min(ahead, len(moves))):
        start(i)
    for i in range(len(moves)):
        load(i).wait()
        store(i).start()
        if i + ahead < len(moves):
            start(i + ahead)
    for i in range(len(moves)):
        if i not in waited:
            store(i).wait()


def move(moves, sources, targets, *, into=()):
    kinds, counts = [], []
    for u in moves:
        a = sources[u.source]
        kind = (u.rows, a.shape[2], a.dtype)
        if kind not in kinds:
            kinds.append(kind)
            counts.append(0)
        u.kind = kinds.index(kind)
        counts[u.kind] += 1
    depth = [min(16, c) for c in counts]
    nbytes = 2 * sum(k[0] * k[1] * k[2].itemsize * c for k, c in zip(kinds, counts))
    hbm = pl.BlockSpec(memory_space=pl.ANY)
    operands = (*sources, *into)
    return pl.pallas_call(
        functools.partial(move_body, moves, kinds, depth, len(operands), len(targets)),
        out_shape=[jax.ShapeDtypeStruct(a.shape, a.dtype) for a in targets],
        in_specs=[hbm] * len(operands),
        out_specs=[hbm] * len(targets),
        input_output_aliases={len(sources) + i: i for i in range(len(into))},
        scratch_shapes=[pltpu.VMEM((d, *k[:2]), k[2]) for d, k in zip(depth, kinds)]
        + [pltpu.SemaphoreType.DMA((len(moves),)), pltpu.SemaphoreType.DMA((len(moves),))],
        compiler_params=pltpu.CompilerParams(vmem_limit_bytes=63 * 2**20),
        cost_estimate=pl.CostEstimate(flops=2 * nbytes, bytes_accessed=nbytes, transcendentals=0),
    )(*operands)


def place_of(c, r, which, part, layer):
    start = c.rows(part)[0]

    def at(chip, core):
        owner = lax.rem(chip + OFFSET[r], CHIPS) * 2 + (core if which == 0 else 1 - core)
        return layer, owner * c.block + start

    return at


def fixed(layer, row=0):
    return lambda chip, core: (layer, row)


def solution(mesh):
    size = mesh.shape["dp"]
    assert size == 2 * CHIPS
    to_right = [(d, (d + 2) % size) for d in range(size)]
    to_left = [(d, (d - 2) % size) for d in range(size)]
    to_other = [(d, d ^ 1) for d in range(size)]

    def step(*arrays):
        terms, weights, m, v = (arrays[i : i + 3] for i in (0, 3, 6, 9))
        chunks, kinds, used = chunks_of([w.shape for w in weights])
        stages = []
        for c in chunks:
            if stages and stages[-1][0].which == c.which and stages[-1][0].half == c.half:
                stages[-1].append(c)
            else:
                stages.append([c])
        for s, stage in enumerate(stages):
            for layer, c in enumerate(stage):
                c.stage = (s, layer)

        results = gather_step(chunks, kinds, used, stages, [t[0] for t in terms], weights, m, v)
        gathered, moments = results[:3], results[3:9]
        for_right, for_left = results[9 : 9 + len(stages)], results[9 + len(stages) :]

        passed, crossed = [], []
        for s in range(len(stages)):
            passed.append((lax.ppermute(for_right[s], "dp", to_right), lax.ppermute(for_left[s], "dp", to_left)))
            crossed.append(tuple(lax.ppermute(p, "dp", to_other) for p in passed[s]))

        whole = []
        for which, g in enumerate(gathered):
            sources, moves = [g], []
            for c in (c for c in chunks if c.which == which):
                stage, layer = c.stage
                if layer == 0:
                    sources += [for_right[stage], for_left[stage]]
                for r in (OWN, LEFT, RIGHT):
                    for core in (0, 1):
                        if core == 0 and r != OWN:
                            for part in "ab":
                                start, stop = c.rows(part)
                                at = place_of(c, r, core, part, c.layer)
                                if (r, part) in ((LEFT, "a"), (RIGHT, "b")):
                                    source = len(sources) - (2 if part == "a" else 1)
                                    moves.append(Move(source, fixed(layer), 0, at, stop - start))
                                else:
                                    moves.append(Move(0, at, 0, at, stop - start))
                        else:
                            at = place_of(c, r, core, "ab", c.layer)
                            moves.append(Move(0, at, 0, at, c.block))
            whole += move(moves, sources, [g])

        moves = []
        for a, array in enumerate(moments):
            layers, rows, _ = array.shape
            for layer in range(layers):
                for row in (0, rows // 2):
                    moves.append(Move(a, fixed(layer, row), a, fixed(layer, row), rows // 2))
        moments = move(moves, moments, moments)

        for s, stage in enumerate(stages):
            which, moves = stage[0].which, []
            for layer, c in enumerate(stage):
                for i in range(4):
                    core, part = i // 2, "ab"[i % 2]
                    start, stop = c.rows(part)
                    moves.append(Move(i, fixed(layer), 0, place_of(c, OPPOSITE, core, part, c.layer), stop - start))
            (whole[which],) = move(moves, [*passed[s], *crossed[s]], [whole[which]], into=[whole[which]])
        return (*whole, *moments)

    all_of, cut = P(None, None, None), P(None, "dp", None)
    return jax.shard_map(
        step,
        mesh=mesh,
        in_specs=(P(("rep", "dp"), None, None, None),) * 3 + (all_of,) * 3 + (cut,) * 6,
        out_specs=(P("rep", None, None),) * 3 + (P("rep", "dp", None),) * 6,
        check_vma=False,
    )
```

```python
import functools

import jax
import jax.numpy as jnp
from jax import lax
from jax.experimental import pallas as pl
from jax.experimental.pallas import tpu as pltpu
from jax.sharding import PartitionSpec as P


MESH = pl.DeviceIdType.MESH
F32, BF16 = jnp.float32, jnp.bfloat16
VMEM_LIMIT = 63 * 2**20
CHIPS = 4
OPPOSITE, RIGHT, LEFT, OWN = range(4)
OFFSET = (2, 1, 3, 0)
FIRST_ROWS = 16
LAST_ROWS = 56


def adamw(w, m, v, g):
    m = 0.9 * m + 0.1 * g
    v = 0.95 * v + 0.05 * g * g
    step = m * lax.rsqrt(v + 1e-8) + 0.1 * w
    return (w - 0.02 * step).astype(BF16), m, v


class Chunk:
    def __init__(self, number, which, layer, kind, place, rows, cols):
        self.number, self.which, self.layer = number, which, layer
        self.kind, self.place = kind, place
        self.rows, self.cols = rows, cols
        self.width = 640 if cols % 640 == 0 else 512
        self.segments = []


def plan(shapes):
    kinds, chunks, used = [], [], []
    for which, (layers, _, rows, cols) in enumerate(shapes):
        if (rows, cols) not in kinds:
            kinds.append((rows, cols))
            used.append(0)
        kind = kinds.index((rows, cols))
        for layer in range(layers):
            chunks.append(Chunk(len(chunks), which, layer, kind, used[kind], rows, cols))
            used[kind] += 1
    stages, count = [], 0
    for c in chunks:
        last = c.which == chunks[-1].which
        cuts = [0, c.rows - LAST_ROWS, c.rows] if c is chunks[-1] else [0, c.rows]
        for start, stop in zip(cuts, cuts[1:]):
            if last or not stages or stages[-1][0][0].which != c.which:
                stages.append([])
            stages[-1].append((c, start, stop - start))
            c.segments.append((count, len(stages) - 1, len(stages[-1]) - 1, start, stop - start))
            count += 1
    return chunks, kinds, used, stages, count


def exchange(chunks, kinds, stages, *refs):
    it = iter(refs)
    take = lambda n: [next(it) for _ in range(n)]
    g, w, m, v = take(3), take(3), take(3), take(3)
    out, new_m, new_v, onward = take(3), take(3), take(3), take(len(stages))
    nk = len(kinds)
    peer, pass_in, near_in, own, w_in, m_in, v_in = (take(nk) for _ in range(7))
    (x_send, x_recv, a_send, a_recv, b_send, b_recv, own_sem, in_sem, out_sem, g_send, g_recv, gx_send, gx_recv) = it
    n = len(chunks)

    me = lax.axis_index("dp")
    chip, core = me // 2, me % 2
    right = lax.rem(chip + 1, CHIPS) * 2 + core
    left = lax.rem(chip + CHIPS - 1, CHIPS) * 2 + core
    other = chip * 2 + (1 - core)
    chip_at = [lax.rem(chip + OFFSET[r], CHIPS) for r in range(4)]
    ahead_chip, behind_chip = (lax.rem(chip + 1 + 2 * (core if s else 1 - core), CHIPS) for s in (1, 0))
    ahead, behind = ahead_chip * 2 + core, behind_chip * 2 + core

    barrier = pltpu.get_barrier_semaphore()
    for d in (right, left, other):
        pl.semaphore_signal(barrier, inc=1, device_id={"dp": d}, device_id_type=MESH)

    pending = []

    def remote(src, dst, send, recv, to):
        copy = pltpu.make_async_remote_copy(
            src_ref=src, dst_ref=dst, send_sem=send, recv_sem=recv, device_id={"dp": to}, device_id_type=MESH)
        copy.start()
        pending.append(copy)
        return copy

    order = [(OPPOSITE, c) for c in chunks]
    for c in chunks:
        order += [(RIGHT, c), (LEFT, c)]
    order += [(OWN, c) for c in chunks]
    slots, seen = {}, [0] * nk
    for r, c in order:
        slots[r, c.number] = seen[c.kind] % 3
        seen[c.kind] += 1

    def own_load(p):
        r, c = order[p]
        return pltpu.make_async_copy(
            g[c.which].at[c.layer, pl.ds((chip_at[r] * 2 + core) * 2, 2)],
            own[c.kind].at[slots[r, c.number]], own_sem.at[r * n + c.number])

    def state_loads(c):
        s = c.place % 2
        return [
            pltpu.make_async_copy(w[c.which].at[c.layer, pl.ds(me * 2, 2)], w_in[c.kind].at[s], in_sem.at[c.number * 3]),
            pltpu.make_async_copy(m[c.which].at[c.layer], m_in[c.kind].at[s], in_sem.at[c.number * 3 + 1]),
            pltpu.make_async_copy(v[c.which].at[c.layer], v_in[c.kind].at[s], in_sem.at[c.number * 3 + 2]),
        ]

    own_load(0).start()
    own_load(1).start()
    pl.semaphore_wait(barrier, 3)

    x = {}

    def swap(r, c):
        x[r, c.number] = remote(
            g[c.which].at[c.layer, pl.ds((chip_at[r] * 2 + (1 - core)) * 2, 2)], peer[c.kind].at[r, c.place],
            x_send.at[r * n + c.number], x_recv.at[r * n + c.number], other)

    first = chunks[0]
    pieces = [(h, rows) for rows in ((0, FIRST_ROWS), (FIRST_ROWS, first.rows)) for h in (0, 1)]
    for k, (h, (start, stop)) in enumerate(pieces):
        s = 4 * n + k
        x[OPPOSITE, h, start] = remote(
            g[first.which].at[first.layer, (chip_at[OPPOSITE] * 2 + (1 - core)) * 2 + h, pl.ds(start, stop - start)],
            peer[first.kind].at[OPPOSITE, first.place, h, pl.ds(start, stop - start)], x_send.at[s], x_recv.at[s], other)
    for c in chunks[1:]:
        swap(OPPOSITE, c)

    position = [0]

    def take_own(r, c):
        p = position[0]
        position[0] += 1
        assert order[p] == (r, c)
        if p + 2 < len(order):
            own_load(p + 2).start()
        own_load(p).wait()
        if (r, c.number) in x:
            x[r, c.number].wait_recv()
        return own[c.kind].at[slots[r, c.number]], peer[c.kind].at[r, c.place]

    def tiles(c, start, stop, body):
        whole = (stop - start) // 16
        cols = [pl.ds(k, c.width) for k in range(0, c.cols, c.width)]

        @pl.loop(0, whole)
        def _(t):
            for k in cols:
                body(pl.ds(pl.multiple_of(start + t * 16, 16), 16), k)

        if start + whole * 16 < stop:
            for k in cols:
                body(pl.ds(start + whole * 16, stop - start - whole * 16), k)

    def add(c, h, mine, theirs, *more, rows=None):
        def tile(r, k):
            total = mine[h, r, k].astype(F32) + theirs[h, r, k].astype(F32)
            for ref in more:
                total += ref[h, r, k].astype(F32)
            theirs[h, r, k] = total.astype(BF16)

        tiles(c, *(rows or (0, c.rows)), tile)

    step0 = {}
    for c in chunks:
        mine, theirs = take_own(OPPOSITE, c)
        for h, (start, stop) in pieces if c is first else [(0, (0, c.rows)), (1, (0, c.rows))]:
            if c is first:
                x[OPPOSITE, h, start].wait_recv()
            add(c, h, mine, theirs, rows=(start, stop))
            s = h * n + c.number if start == 0 else 2 * n + h
            step0.setdefault((h, c.number), []).append(remote(
                theirs.at[h, pl.ds(start, stop - start)], pass_in[c.kind].at[c.place, h, pl.ds(start, stop - start)],
                a_send.at[s], a_recv.at[s], (right, left)[h]))
        swap(RIGHT, c)
        swap(LEFT, c)

    step1 = {}
    for c in chunks:
        for r, to, side in ((RIGHT, right, 0), (LEFT, left, 1)):
            mine, theirs = take_own(r, c)
            for h in (side, 1 - side):
                if h == side:
                    for copy in step0[h, c.number]:
                        copy.wait_recv()
                    add(c, h, mine, theirs, pass_in[c.kind].at[c.place])
                else:
                    add(c, h, mine, theirs)
                s = (side * n + c.number) * 2 + h
                step1[side, c.number, h] = remote(
                    theirs.at[h], near_in[c.kind].at[side, c.place, h], b_send.at[s], b_recv.at[s], to)
        swap(OWN, c)

    for c in chunks[:2]:
        for copy in state_loads(c):
            copy.start()
    arrivals, crossing, stores = {}, [], {}
    for c in chunks:
        mine, theirs = take_own(OWN, c)
        for copy in state_loads(c):
            copy.wait()
        s = c.place % 2
        from_left, from_right = near_in[c.kind].at[0, c.place], near_in[c.kind].at[1, c.place]
        w_ref, m_ref, v_ref = w_in[c.kind].at[s], m_in[c.kind].at[s], v_in[c.kind].at[s]
        for h in (0, 1):
            step1[0, c.number, h].wait_recv()
            step1[1, c.number, h].wait_recv()

            def tile(r, k):
                total = mine[h, r, k].astype(F32) + theirs[h, r, k].astype(F32)
                total += from_left[h, r, k].astype(F32) + from_right[h, r, k].astype(F32)
                gradient = total.astype(BF16).astype(F32)
                new = adamw(w_ref[h, r, k].astype(F32), m_ref[h, r, k], v_ref[h, r, k], gradient)
                theirs[h, r, k], m_ref[h, r, k], v_ref[h, r, k] = new

            tiles(c, 0, c.rows, tile)
        for number, stage, index, start, size in c.segments:
            rows = pl.ds(start, size)
            for k, (h, to) in enumerate(((core, ahead), (1 - core, ahead), (1 - core, behind), (core, behind))):
                dst = onward[stage].at[index, core] if k == 0 else out[c.which].at[c.layer, me * 2 + h, rows]
                arrivals[number, k] = remote(
                    theirs.at[h, rows], dst, g_send.at[number * 4 + k], g_recv.at[number * 4 + k], to)
        target = out[c.which].at[c.layer, pl.ds(me * 2, 2)]
        crossing.append(remote(theirs, target, gx_send.at[c.number], gx_recv.at[c.number], other))
        stores[c.number] = [
            pltpu.make_async_copy(theirs, target, out_sem.at[c.number * 3]),
            pltpu.make_async_copy(m_ref, new_m[c.which].at[c.layer], out_sem.at[c.number * 3 + 1]),
            pltpu.make_async_copy(v_ref, new_v[c.which].at[c.layer], out_sem.at[c.number * 3 + 2]),
        ]
        for copy in stores[c.number]:
            copy.start()
        if c.number + 1 < n and c.number >= 1:
            following = chunks[c.number + 1]
            for before in chunks[: c.number]:
                if before.kind == following.kind and before.place == following.place - 2:
                    for copy in stores.pop(before.number):
                        copy.wait()
            for copy in state_loads(following):
                copy.start()

    for c in chunks:
        for number, stage, index, start, size in c.segments:
            rows = pl.ds(start, size)
            for k, (h, owner) in enumerate(
                ((core, behind_chip), (1 - core, behind_chip), (1 - core, ahead_chip), (core, ahead_chip))):
                s = n + number * 4 + k
                arrivals[number, k].wait_recv()
                there = out[c.which].at[c.layer, (owner * 2 + core) * 2 + h, rows]
                crossing.append(remote(
                    onward[stage].at[index, core] if k == 0 else there,
                    onward[stage].at[index, core] if k == 2 else there, gx_send.at[s], gx_recv.at[s], other))
    for copy in crossing:
        copy.wait_recv()
    for copies in stores.values():
        for copy in copies:
            copy.wait()
    for copy in pending:
        copy.wait_send()


def gather_step(chunks, kinds, used, stages, segments, terms, weights, m, v):
    n = len(chunks)
    hbm = pl.BlockSpec(memory_space=pltpu.HBM)
    slots = lambda lead, dtype: [
        pltpu.VMEM((*(u if x is None else x for x in lead), 2, *k), dtype) for k, u in zip(kinds, used)]
    dma = lambda count: pltpu.SemaphoreType.DMA((count,))
    results = [jax.ShapeDtypeStruct(w.shape, BF16) for w in weights]
    results += [jax.ShapeDtypeStruct(a.shape, F32) for a in (*m, *v)]
    results += [jax.ShapeDtypeStruct((len(s), 2, s[0][2], s[0][0].cols), BF16) for s in stages]
    return pl.pallas_call(
        functools.partial(exchange, chunks, kinds, stages),
        out_shape=results,
        in_specs=[hbm] * 12,
        out_specs=[hbm] * len(results),
        scratch_shapes=[
            *slots((4, None), BF16), *slots((None,), BF16), *slots((2, None), BF16), *slots((3,), BF16),
            *slots((2,), BF16), *slots((2,), F32), *slots((2,), F32),
            dma(4 * n + 4), dma(4 * n + 4), dma(2 * n + 2), dma(2 * n + 2), dma(4 * n), dma(4 * n), dma(4 * n), dma(3 * n),
            dma(3 * n), dma(4 * segments), dma(4 * segments), dma(n + 4 * segments), dma(n + 4 * segments),
        ],
        compiler_params=pltpu.CompilerParams(collective_id=0, has_side_effects=True, vmem_limit_bytes=VMEM_LIMIT),
    )(*terms, *weights, *m, *v)


class Move:
    def __init__(self, source, source_at, target, target_at, shape):
        self.source, self.source_at = source, source_at
        self.target, self.target_at = target, target_at
        self.shape = shape


def move_body(moves, kinds, depth, n_in, n_out, *refs):
    sources, targets = refs[:n_in], refs[n_in : n_in + n_out]
    bufs, (in_sem, out_sem) = refs[n_in + n_out : -2], refs[-2:]
    me = lax.axis_index("dp")
    chip, core = me // 2, me % 2
    seen, place = [0] * len(kinds), []
    for u in moves:
        place.append((u.kind, seen[u.kind] % depth[u.kind]))
        seen[u.kind] += 1

    def load(i):
        u, (kind, slot) = moves[i], place[i]
        return pltpu.make_async_copy(sources[u.source].at[u.source_at(chip, core)], bufs[kind].at[slot], in_sem.at[i])

    def store(i):
        u, (kind, slot) = moves[i], place[i]
        return pltpu.make_async_copy(bufs[kind].at[slot], targets[u.target].at[u.target_at(chip, core)], out_sem.at[i])

    waited, last = set(), {}

    def start(i):
        if place[i] in last:
            store(last[place[i]]).wait()
            waited.add(last[place[i]])
        last[place[i]] = i
        load(i).start()

    ahead = 8
    for i in range(min(ahead, len(moves))):
        start(i)
    for i in range(len(moves)):
        load(i).wait()
        store(i).start()
        if i + ahead < len(moves):
            start(i + ahead)
    for i in range(len(moves)):
        if i not in waited:
            store(i).wait()


def move(moves, sources, targets):
    kinds, counts = [], []
    for u in moves:
        kind = (u.shape, sources[u.source].dtype)
        if kind not in kinds:
            kinds.append(kind)
            counts.append(0)
        u.kind = kinds.index(kind)
        counts[u.kind] += 1
    depth = [min(14, c) for c in counts]
    size = lambda shape: functools.reduce(lambda a, b: a * b, shape)
    nbytes = 2 * sum(size(shape) * dtype.itemsize * c for (shape, dtype), c in zip(kinds, counts))
    hbm = pl.BlockSpec(memory_space=pltpu.HBM)
    return pl.pallas_call(
        functools.partial(move_body, moves, kinds, depth, len(sources), len(targets)),
        out_shape=[jax.ShapeDtypeStruct(a.shape, a.dtype) for a in targets],
        in_specs=[hbm] * len(sources),
        out_specs=[hbm] * len(targets),
        scratch_shapes=[pltpu.VMEM((d, *shape), dtype) for d, (shape, dtype) in zip(depth, kinds)]
        + [pltpu.SemaphoreType.DMA((len(moves),)), pltpu.SemaphoreType.DMA((len(moves),))],
        compiler_params=pltpu.CompilerParams(vmem_limit_bytes=48 * 2**20),
        cost_estimate=pl.CostEstimate(flops=2 * nbytes, bytes_accessed=nbytes, transcendentals=0),
    )(*sources)


def put_body(moves, n_in, *refs):
    sources, target, sem = refs[:n_in], refs[-2], refs[-1]
    me = lax.axis_index("dp")
    chip, core = me // 2, me % 2
    copies = [
        pltpu.make_async_copy(
            sources[u.source].at[u.source_at(chip, core)], target.at[u.target_at(chip, core)], sem.at[i])
        for i, u in enumerate(moves)
    ]
    for copy in copies:
        copy.start()
    for copy in copies:
        copy.wait()


def put(moves, sources, into):
    nbytes = 2 * sum(a.size * a.dtype.itemsize for a in sources)
    hbm = pl.BlockSpec(memory_space=pltpu.HBM)
    return pl.pallas_call(
        functools.partial(put_body, moves, len(sources) + 1),
        out_shape=jax.ShapeDtypeStruct(into.shape, into.dtype),
        in_specs=[pl.BlockSpec(memory_space=pltpu.VMEM)] * len(sources) + [hbm],
        out_specs=hbm,
        input_output_aliases={len(sources): 0},
        scratch_shapes=[pltpu.SemaphoreType.DMA((len(moves),))],
        compiler_params=pltpu.CompilerParams(vmem_limit_bytes=16 * 2**20),
        cost_estimate=pl.CostEstimate(flops=2 * nbytes, bytes_accessed=nbytes, transcendentals=0),
    )(*sources, into)


def known_moves(chunks, which, source, onward, target):
    def block(c, r, parity):
        def at(chip, core):
            owner = lax.rem(chip + (0 if r == OWN else 1 + 2 * core), CHIPS) * 2 + parity
            return c.layer, pl.ds(owner * 2, 2)

        return at

    def behind(c, parity, passed, start, size):
        def at(chip, core):
            owner = lax.rem(chip + 3 - 2 * core, CHIPS) * 2 + parity
            return c.layer, owner * 2 + (core if passed else 1 - core), pl.ds(start, size)

        return at

    moves = []
    for c in (c for c in chunks if c.which == which):
        for parity in (0, 1):
            for r in (OWN, RIGHT):
                at = block(c, r, parity)
                moves.append(Move(source, at, target, at, (2, c.rows, c.cols)))
            at = behind(c, parity, False, 0, c.rows)
            moves.append(Move(source, at, target, at, (c.rows, c.cols)))
            for _, stage, index, start, size in c.segments:
                at = lambda chip, core, index=index, parity=parity: (index, parity)
                moves.append(Move(onward[stage], at, target, behind(c, parity, True, start, size), (size, c.cols)))
    return moves


def last_moves(stage, sources, target):
    moves = []
    for index, (c, start, size) in enumerate(stage):
        for k, source in enumerate(sources):
            for parity in (0, 1):
                def to(chip, core, c=c, start=start, size=size, k=k, parity=parity):
                    owner = lax.rem(chip + 2, CHIPS) * 2 + parity
                    return c.layer, owner * 2 + (core if k == 0 else 1 - core), pl.ds(start, size)

                at = lambda chip, core, index=index, parity=parity: (index, parity)
                moves.append(Move(source, at, target, to, (size, c.cols)))
    return moves


def solution(mesh):
    devices = mesh.shape["dp"]
    assert devices == 2 * CHIPS
    onward_to = [(d, (d + 2 - 4 * (d % 2)) % devices) for d in range(devices)]
    across = [(d, d ^ 1) for d in range(devices)]

    def halves(a, count):
        return a.reshape(a.shape[0], count, a.shape[1] // count, a.shape[2])

    def step(*arrays):
        shapes = [a.shape for a in arrays]
        terms = [halves(t[0], 2 * devices) for t in arrays[:3]]
        weights = [halves(w, 2 * devices) for w in arrays[3:6]]
        m, v = ([halves(a, 2) for a in arrays[i : i + 3]] for i in (6, 9))
        chunks, kinds, used, stages, segments = plan([w.shape for w in weights])
        results = gather_step(chunks, kinds, used, stages, segments, terms, weights, m, v)
        gathered, moments, onward = results[:3], results[3:9], results[9:]

        passed, crossed = [], []
        for s, piece in enumerate(onward):
            passed.append(lax.ppermute(piece, "dp", onward_to))
            crossed.append(lax.ppermute(passed[s], "dp", across))

        whole = [None] * 3
        sources = [*gathered[:2], *onward[:2]]
        moves = [u for i in (0, 1) for u in known_moves(chunks, i, i, [2, 3], i)]
        whole[:2] = move(moves, sources, gathered[:2])
        sources = [gathered[2], *onward[2:], *moments]
        moves = known_moves(chunks, 2, 0, [None, None, *range(1, len(stages) - 1)], 0)
        for a, array in enumerate(moments):
            for layer in range(array.shape[0]):
                for h in (0, 1):
                    at = lambda chip, core, layer=layer, h=h: (layer, h)
                    moves.append(Move(len(stages) - 1 + a, at, 1 + a, at, array.shape[2:]))
        whole[2], *moments = move(moves, sources, [gathered[2], *moments])

        for group in ([0], [1], [2], range(3, len(stages))):
            which = stages[group[0]][0][0].which
            sources, moves = [], []
            for s in group:
                moves += last_moves(stages[s], (len(sources), len(sources) + 1), 0)
                sources += [passed[s], crossed[s]]
            whole[which] = put(moves, sources, whole[which])
        return tuple(a.reshape(s) for a, s in zip((*whole, *moments), shapes[3:]))

    all_of, cut = P(None, None, None), P(None, "dp", None)
    return jax.shard_map(
        step,
        mesh=mesh,
        in_specs=(P(("rep", "dp"), None, None, None),) * 3 + (all_of,) * 3 + (cut,) * 6,
        out_specs=(P("rep", None, None),) * 3 + (P("rep", "dp", None),) * 6,
        check_vma=False,
    )
```

```python
import functools

import jax
import jax.numpy as jnp
from jax import lax
from jax.experimental import pallas as pl
from jax.experimental.pallas import tpu as pltpu
from jax.sharding import PartitionSpec as P


MESH = pl.DeviceIdType.MESH
F32, BF16 = jnp.float32, jnp.bfloat16
VMEM_LIMIT = 63 * 2**20
CHIPS = 4
OPPOSITE, RIGHT, LEFT, OWN = range(4)
OFFSET = (2, 1, 3, 0)
FIRST_ROWS = 16
LAST_ROWS = 56


def adamw(w, m, v, g):
    m = 0.9 * m + 0.1 * g
    v = 0.95 * v + 0.05 * g * g
    step = m * lax.rsqrt(v + 1e-8) + 0.1 * w
    return (w - 0.02 * step).astype(BF16), m, v


class Chunk:
    def __init__(self, number, which, layer, kind, place, rows, cols):
        self.number, self.which, self.layer = number, which, layer
        self.kind, self.place = kind, place
        self.rows, self.cols = rows, cols
        self.width = 640 if cols % 640 == 0 else 512
        self.segments = []


def plan(shapes):
    kinds, chunks, used = [], [], []
    for which, (layers, _, rows, cols) in enumerate(shapes):
        if (rows, cols) not in kinds:
            kinds.append((rows, cols))
            used.append(0)
        kind = kinds.index((rows, cols))
        for layer in range(layers):
            chunks.append(Chunk(len(chunks), which, layer, kind, used[kind], rows, cols))
            used[kind] += 1
    stages, count = [], 0
    for c in chunks:
        last = c.which == chunks[-1].which
        cuts = [0, c.rows - LAST_ROWS, c.rows] if c is chunks[-1] else [0, c.rows]
        for start, stop in zip(cuts, cuts[1:]):
            if last or not stages or stages[-1][0][0].which != c.which:
                stages.append([])
            stages[-1].append((c, start, stop - start))
            c.segments.append((count, len(stages) - 1, len(stages[-1]) - 1, start, stop - start))
            count += 1
    return chunks, kinds, used, stages, count


def exchange(chunks, kinds, stages, segments, *refs):
    it = iter(refs)
    take = lambda n: [next(it) for _ in range(n)]
    g, w, m, v = take(3), take(3), take(3), take(3)
    out, new_m, new_v, onward = take(3), take(3), take(3), take(len(stages))
    nk = len(kinds)
    peer, pass_in, near_in, own, w_in, m_in, v_in = (take(nk) for _ in range(7))
    (first_in, first_sem, x_send, x_recv, a_send, a_recv, b_send, b_recv, own_sem, in_sem, out_sem, kept_sem, g_send, g_recv,
     gx_send, gx_recv) = it
    n = len(chunks)

    me = lax.axis_index("dp")
    chip, core = me // 2, me % 2
    right = lax.rem(chip + 1, CHIPS) * 2 + core
    left = lax.rem(chip + CHIPS - 1, CHIPS) * 2 + core
    other = chip * 2 + (1 - core)
    chip_at = [lax.rem(chip + OFFSET[r], CHIPS) for r in range(4)]
    ahead_chip, behind_chip = (lax.rem(chip + 1 + 2 * (core if s else 1 - core), CHIPS) for s in (1, 0))
    ahead, behind = ahead_chip * 2 + core, behind_chip * 2 + core

    barrier = pltpu.get_barrier_semaphore()
    for d in (right, left, other):
        pl.semaphore_signal(barrier, inc=1, device_id={"dp": d}, device_id_type=MESH)

    def remote(src, dst, send, recv, to):
        pltpu.make_async_remote_copy(
            src_ref=src, dst_ref=dst, send_sem=send, recv_sem=recv, device_id={"dp": to}, device_id_type=MESH).start()

    def await_bytes(ref, sem):
        pltpu.make_async_copy(ref, ref, sem).wait()

    order = [(OPPOSITE, c) for c in chunks]
    for c in chunks:
        order += [(RIGHT, c), (LEFT, c)]
    order += [(OWN, c) for c in chunks]
    slots, seen = {}, [0] * nk
    for r, c in order:
        slots[r, c.number] = seen[c.kind] % 3
        seen[c.kind] += 1

    def own_load(p):
        r, c = order[p]
        slot = slots[r, c.number]
        return pltpu.make_async_copy(
            g[c.which].at[c.layer, pl.ds((chip_at[r] * 2 + core) * 2, 2)], own[c.kind].at[slot], own_sem.at[c.kind * 3 + slot])

    def load_state(c):
        s = c.place % 2
        sem = (c.kind * 2 + s) * 2
        pltpu.make_async_copy(w[c.which].at[c.layer, pl.ds(me * 2, 2)], w_in[c.kind].at[s], in_sem.at[sem]).start()
        pltpu.make_async_copy(m[c.which].at[c.layer], m_in[c.kind].at[s], in_sem.at[sem + 1]).start()
        pltpu.make_async_copy(v[c.which].at[c.layer], v_in[c.kind].at[s], in_sem.at[sem + 1]).start()

    first = chunks[0]
    pieces = [(h, rows) for rows in ((0, FIRST_ROWS), (FIRST_ROWS, first.rows)) for h in (0, 1)]

    def given(h, start, stop):
        return g[first.which].at[first.layer, (chip_at[OPPOSITE] * 2 + (1 - core)) * 2 + h, pl.ds(start, stop - start)]

    for h in (0, 1):
        pltpu.make_async_copy(given(h, 0, FIRST_ROWS), first_in.at[h], first_sem.at[0]).start()
    own_load(0).start()
    own_load(1).start()
    await_bytes(first_in, first_sem.at[0])
    pl.semaphore_wait(barrier, 3)

    def swap(r, c):
        remote(
            g[c.which].at[c.layer, pl.ds((chip_at[r] * 2 + (1 - core)) * 2, 2)], peer[c.kind].at[r, c.place],
            x_send.at[c.kind], x_recv.at[{OPPOSITE: 0, RIGHT: n, LEFT: n, OWN: 2 * n}[r] + c.number], other)

    def first_piece(h, start, stop):
        return peer[first.kind].at[OPPOSITE, first.place, h, pl.ds(start, stop - start)]

    for k, (h, (start, stop)) in enumerate(pieces):
        remote(
            first_in.at[h] if start == 0 else given(h, start, stop), first_piece(h, start, stop),
            x_send.at[first.kind], x_recv.at[3 * n + k], other)
    for c in chunks[1:]:
        swap(OPPOSITE, c)

    position = [0]

    def take_own(r, c):
        p = position[0]
        position[0] += 1
        assert order[p] == (r, c)
        if p + 2 < len(order):
            own_load(p + 2).start()
        own_load(p).wait()
        if r == RIGHT:
            await_bytes(peer[c.kind].at[pl.ds(RIGHT, 2), c.place], x_recv.at[n + c.number])
        elif r == OWN or r == OPPOSITE and c is not first:
            await_bytes(peer[c.kind].at[r, c.place], x_recv.at[(0 if r == OPPOSITE else 2 * n) + c.number])
        return own[c.kind].at[slots[r, c.number]], peer[c.kind].at[r, c.place]

    def tiles(c, start, stop, body):
        whole = (stop - start) // 16
        cols = [pl.ds(k, c.width) for k in range(0, c.cols, c.width)]

        @pl.loop(0, whole)
        def _(t):
            for k in cols:
                body(pl.ds(pl.multiple_of(start + t * 16, 16), 16), k)

        if start + whole * 16 < stop:
            for k in cols:
                body(pl.ds(start + whole * 16, stop - start - whole * 16), k)

    def add(c, h, mine, theirs, *more, rows=None):
        def tile(r, k):
            total = mine[h, r, k].astype(F32) + theirs[h, r, k].astype(F32)
            for ref in more:
                total += ref[h, r, k].astype(F32)
            theirs[h, r, k] = total.astype(BF16)

        tiles(c, *(rows or (0, c.rows)), tile)

    for c in chunks:
        mine, theirs = take_own(OPPOSITE, c)
        for k, (h, (start, stop)) in enumerate(pieces if c is first else [(0, (0, c.rows)), (1, (0, c.rows))]):
            if c is first:
                await_bytes(first_piece(h, start, stop), x_recv.at[3 * n + k])
            add(c, h, mine, theirs, rows=(start, stop))
            remote(
                theirs.at[h, pl.ds(start, stop - start)], pass_in[c.kind].at[c.place, h, pl.ds(start, stop - start)],
                a_send.at[c.kind], a_recv.at[c.number], (right, left)[h])
        swap(RIGHT, c)
        swap(LEFT, c)

    for c in chunks:
        for r, to, side in ((RIGHT, right, 0), (LEFT, left, 1)):
            mine, theirs = take_own(r, c)
            if r == RIGHT:
                await_bytes(pass_in[c.kind].at[c.place], a_recv.at[c.number])
            for h in (side, 1 - side):
                add(c, h, mine, theirs, *([pass_in[c.kind].at[c.place]] if h == side else []))
                remote(theirs.at[h], near_in[c.kind].at[side, c.place, h], b_send.at[c.kind], b_recv.at[c.number], to)
        swap(OWN, c)

    for c in chunks[:2]:
        load_state(c)
    storing = []

    def await_moments(c):
        await_bytes(m_in[c.kind], out_sem.at[c.kind * 2 + c.place % 2])

    for c in chunks:
        mine, theirs = take_own(OWN, c)
        s = c.place % 2
        await_bytes(w_in[c.kind].at[s], in_sem.at[(c.kind * 2 + s) * 2])
        await_bytes(m_in[c.kind], in_sem.at[(c.kind * 2 + s) * 2 + 1])
        await_bytes(near_in[c.kind].at[:, c.place], b_recv.at[c.number])
        from_left, from_right = near_in[c.kind].at[0, c.place], near_in[c.kind].at[1, c.place]
        w_ref, m_ref, v_ref = w_in[c.kind].at[s], m_in[c.kind].at[s], v_in[c.kind].at[s]
        for h in (0, 1):

            def tile(r, k):
                total = mine[h, r, k].astype(F32) + theirs[h, r, k].astype(F32)
                total += from_left[h, r, k].astype(F32) + from_right[h, r, k].astype(F32)
                gradient = total.astype(BF16).astype(F32)
                new = adamw(w_ref[h, r, k].astype(F32), m_ref[h, r, k], v_ref[h, r, k], gradient)
                theirs[h, r, k], m_ref[h, r, k], v_ref[h, r, k] = new

            tiles(c, 0, c.rows, tile)
        for number, stage, index, start, size in c.segments:
            rows = pl.ds(start, size)
            for k, (h, to) in enumerate(((core, ahead), (1 - core, ahead), (1 - core, behind), (core, behind))):
                dst = onward[stage].at[index, core] if k == 0 else out[c.which].at[c.layer, me * 2 + h, rows]
                if number == segments - 1:
                    dst = onward[stage].at[k]
                remote(theirs.at[h, rows], dst, g_send.at[c.kind], g_recv.at[number], to)
        target = out[c.which].at[c.layer, pl.ds(me * 2, 2)]
        remote(theirs, target, gx_send.at[c.kind], gx_recv.at[c.kind], other)
        pltpu.make_async_copy(theirs, target, kept_sem.at[c.kind]).start()
        pltpu.make_async_copy(m_ref, new_m[c.which].at[c.layer], out_sem.at[c.kind * 2 + s]).start()
        pltpu.make_async_copy(v_ref, new_v[c.which].at[c.layer], out_sem.at[c.kind * 2 + s]).start()
        storing.append(c)
        if 1 <= c.number < n - 1:
            following = chunks[c.number + 1]
            for before in storing[:-1]:
                if before.kind == following.kind and before.place == following.place - 2:
                    await_moments(before)
                    storing.remove(before)
            load_state(following)

    several = {}
    for c in chunks:
        for number, stage, index, start, size in c.segments:
            rows = pl.ds(start, size)
            await_bytes(near_in[c.kind].at[:, c.place, :, rows], g_recv.at[number])
            if number == segments - 1:
                continue
            sem = nk + (c.kind if size == c.rows else nk)
            several.setdefault(sem, []).append((c, rows))
            for k, (h, owner) in enumerate(
                ((core, behind_chip), (1 - core, behind_chip), (1 - core, ahead_chip), (core, ahead_chip))):
                there = out[c.which].at[c.layer, (owner * 2 + core) * 2 + h, rows]
                remote(
                    onward[stage].at[index, core] if k == 0 else there,
                    onward[stage].at[index, core] if k == 2 else there, gx_send.at[sem], gx_recv.at[sem], other)
    for c in storing:
        await_moments(c)
    for kind in range(nk):
        await_bytes(peer[kind], x_send.at[kind])
        await_bytes(peer[kind].at[0], a_send.at[kind])
        await_bytes(peer[kind].at[pl.ds(1, 2)], b_send.at[kind])
        await_bytes(peer[kind].at[pl.ds(0, 2)], g_send.at[kind])
        await_bytes(peer[kind].at[0], gx_send.at[kind])
        await_bytes(peer[kind].at[0], gx_recv.at[kind])
        await_bytes(peer[kind].at[0], kept_sem.at[kind])
    for sem, parts in several.items():
        c, rows = parts[0]
        for sems in (gx_send, gx_recv):
            await_bytes(near_in[c.kind].at[:, pl.ds(0, len(parts)), :, rows], sems.at[sem])


def gather_step(chunks, kinds, used, stages, segments, terms, weights, m, v):
    n, nk = len(chunks), len(kinds)
    hbm = pl.BlockSpec(memory_space=pltpu.HBM)
    slots = lambda lead, dtype: [
        pltpu.VMEM((*(u if x is None else x for x in lead), 2, *k), dtype) for k, u in zip(kinds, used)]
    dma = lambda count: pltpu.SemaphoreType.DMA((count,))
    results = [jax.ShapeDtypeStruct(w.shape, BF16) for w in weights]
    results += [jax.ShapeDtypeStruct(a.shape, F32) for a in (*m, *v)]
    results += [jax.ShapeDtypeStruct((len(s), 2, s[0][2], s[0][0].cols), BF16) for s in stages[:-1]]
    results += [jax.ShapeDtypeStruct((4, s[0][2], s[0][0].cols), BF16) for s in stages[-1:]]
    return pl.pallas_call(
        functools.partial(exchange, chunks, kinds, stages, segments),
        out_shape=results,
        in_specs=[hbm] * 12,
        out_specs=[hbm] * len(results),
        scratch_shapes=[
            *slots((4, None), BF16), *slots((None,), BF16), *slots((2, None), BF16), *slots((3,), BF16),
            *slots((2,), BF16), *slots((2,), F32), *slots((2,), F32),
            pltpu.VMEM((2, FIRST_ROWS, chunks[0].cols), BF16), dma(1),
            dma(nk), dma(3 * n + 4), dma(nk), dma(n), dma(nk), dma(n), dma(3 * nk), dma(4 * nk), dma(2 * nk), dma(nk),
            dma(nk), dma(segments), dma(2 * nk + 1), dma(2 * nk + 1),
        ],
        compiler_params=pltpu.CompilerParams(collective_id=0, has_side_effects=True, vmem_limit_bytes=VMEM_LIMIT),
    )(*terms, *weights, *m, *v)


class Move:
    def __init__(self, source, source_at, target, target_at, shape):
        self.source, self.source_at = source, source_at
        self.target, self.target_at = target, target_at
        self.shape = shape


def move_body(moves, kinds, depth, n_in, n_out, *refs):
    sources, targets = refs[:n_in], refs[n_in : n_in + n_out]
    bufs, (in_sem, out_sem) = refs[n_in + n_out : -2], refs[-2:]
    me = lax.axis_index("dp")
    chip, core = me // 2, me % 2
    seen, place = [0] * len(kinds), []
    for u in moves:
        place.append((u.kind, seen[u.kind] % depth[u.kind]))
        seen[u.kind] += 1

    def load(i):
        u, (kind, slot) = moves[i], place[i]
        return pltpu.make_async_copy(sources[u.source].at[u.source_at(chip, core)], bufs[kind].at[slot], in_sem.at[i])

    def store(i):
        u, (kind, slot) = moves[i], place[i]
        return pltpu.make_async_copy(bufs[kind].at[slot], targets[u.target].at[u.target_at(chip, core)], out_sem.at[i])

    waited, last = set(), {}

    def start(i):
        if place[i] in last:
            store(last[place[i]]).wait()
            waited.add(last[place[i]])
        last[place[i]] = i
        load(i).start()

    ahead = 8
    for i in range(min(ahead, len(moves))):
        start(i)
    for i in range(len(moves)):
        load(i).wait()
        store(i).start()
        if i + ahead < len(moves):
            start(i + ahead)
    for i in range(len(moves)):
        if i not in waited:
            store(i).wait()


def move(moves, sources, targets):
    kinds, counts = [], []
    for u in moves:
        kind = (u.shape, sources[u.source].dtype)
        if kind not in kinds:
            kinds.append(kind)
            counts.append(0)
        u.kind = kinds.index(kind)
        counts[u.kind] += 1
    depth = [min(14, c) for c in counts]
    size = lambda shape: functools.reduce(lambda a, b: a * b, shape)
    nbytes = 2 * sum(size(shape) * dtype.itemsize * c for (shape, dtype), c in zip(kinds, counts))
    hbm = pl.BlockSpec(memory_space=pltpu.HBM)
    return pl.pallas_call(
        functools.partial(move_body, moves, kinds, depth, len(sources), len(targets)),
        out_shape=[jax.ShapeDtypeStruct(a.shape, a.dtype) for a in targets],
        in_specs=[hbm] * len(sources),
        out_specs=[hbm] * len(targets),
        scratch_shapes=[pltpu.VMEM((d, *shape), dtype) for d, (shape, dtype) in zip(depth, kinds)]
        + [pltpu.SemaphoreType.DMA((len(moves),)), pltpu.SemaphoreType.DMA((len(moves),))],
        compiler_params=pltpu.CompilerParams(vmem_limit_bytes=48 * 2**20),
        cost_estimate=pl.CostEstimate(flops=2 * nbytes, bytes_accessed=nbytes, transcendentals=0),
    )(*sources)


def put_body(moves, n_in, *refs):
    sources, target, sem = refs[:n_in], refs[-2], refs[-1]
    me = lax.axis_index("dp")
    chip, core = me // 2, me % 2
    copies = [
        pltpu.make_async_copy(
            sources[u.source].at[u.source_at(chip, core)], target.at[u.target_at(chip, core)], sem.at[i])
        for i, u in enumerate(moves)
    ]
    for copy in copies:
        copy.start()
    for copy in copies:
        copy.wait()


def put(moves, sources, into):
    nbytes = 2 * sum(a.size * a.dtype.itemsize for a in sources)
    hbm = pl.BlockSpec(memory_space=pltpu.HBM)
    return pl.pallas_call(
        functools.partial(put_body, moves, len(sources) + 1),
        out_shape=jax.ShapeDtypeStruct(into.shape, into.dtype),
        in_specs=[pl.BlockSpec(memory_space=pltpu.VMEM)] * len(sources) + [hbm],
        out_specs=hbm,
        input_output_aliases={len(sources): 0},
        scratch_shapes=[pltpu.SemaphoreType.DMA((len(moves),))],
        compiler_params=pltpu.CompilerParams(vmem_limit_bytes=16 * 2**20),
        cost_estimate=pl.CostEstimate(flops=2 * nbytes, bytes_accessed=nbytes, transcendentals=0),
    )(*sources, into)


def known_moves(chunks, which, source, onward, target):
    def block(c, r, parity, size):
        def at(chip, core):
            owner = lax.rem(chip + (0 if r == OWN else 1 + 2 * core), CHIPS) * 2 + parity
            return c.layer, pl.ds(owner * 2, 2), pl.ds(0, size)

        return at

    def behind(c, parity, passed, start, size):
        def at(chip, core):
            owner = lax.rem(chip + 3 - 2 * core, CHIPS) * 2 + parity
            return c.layer, owner * 2 + (core if passed else 1 - core), pl.ds(start, size)

        return at

    moves = []
    for c in (c for c in chunks if c.which == which):
        segments = [segment for segment in c.segments if onward[segment[1]] is not None]
        known = sum(segment[-1] for segment in segments)
        for parity in (0, 1):
            for r, size in ((OWN, c.rows), (RIGHT, known)):
                at = block(c, r, parity, size)
                moves.append(Move(source, at, target, at, (2, size, c.cols)))
            at = behind(c, parity, False, 0, known)
            moves.append(Move(source, at, target, at, (known, c.cols)))
            for _, stage, index, start, size in segments:
                at = lambda chip, core, index=index, parity=parity: (index, parity)
                moves.append(Move(onward[stage], at, target, behind(c, parity, True, start, size), (size, c.cols)))
    return moves


def late_moves(stage, sources, target):
    (c, start, size), moves = stage[0], []
    for k, source in enumerate(sources):
        for i in range(4):
            def to(chip, core, k=k, i=i):
                there = core if k == 0 else 1 - core
                owner = lax.rem(chip + (3 - 2 * there if i < 2 else 1 + 2 * there), CHIPS) * 2 + there
                return c.layer, owner * 2 + (there if i in (0, 3) else 1 - there), pl.ds(start, size)

            moves.append(Move(source, lambda chip, core, i=i: (i,), target, to, (size, c.cols)))
    return moves


def last_moves(stage, sources, target, joined=False):
    moves = []
    for index, (c, start, size) in enumerate(stage):
        for k, source in enumerate(sources):
            for parity in (0, 1):
                def to(chip, core, c=c, start=start, size=size, k=k, parity=parity):
                    half = core if k == 0 else 1 - core
                    owner = lax.rem(chip + 2, CHIPS) * 2 + ((half if parity == 0 else 1 - half) if joined else parity)
                    return c.layer, owner * 2 + half, pl.ds(start, size)

                at = lambda chip, core, index=index, parity=parity: (index, parity)
                moves.append(Move(source, at, target, to, (size, c.cols)))
    return moves


def solution(mesh):
    devices = mesh.shape["dp"]
    assert devices == 2 * CHIPS
    onward_to = [(d, (d + 2 - 4 * (d % 2)) % devices) for d in range(devices)]
    across = [(d, d ^ 1) for d in range(devices)]

    def halves(a, count):
        return a.reshape(a.shape[0], count, a.shape[1] // count, a.shape[2])

    def step(*arrays):
        shapes = [a.shape for a in arrays]
        terms = [halves(t[0], 2 * devices) for t in arrays[:3]]
        weights = [halves(w, 2 * devices) for w in arrays[3:6]]
        m, v = ([halves(a, 2) for a in arrays[i : i + 3]] for i in (6, 9))
        chunks, kinds, used, stages, segments = plan([w.shape for w in weights])
        results = gather_step(chunks, kinds, used, stages, segments, terms, weights, m, v)
        gathered, moments, onward = results[:3], results[3:9], list(results[9:])

        late = onward[-1], lax.ppermute(onward[-1], "dp", across)
        onward[-1] = jnp.stack([late[0][0], late[1][2]])[None]
        passed, crossed = [], []
        for s, piece in enumerate(onward):
            passed.append(lax.ppermute(piece, "dp", onward_to))
            crossed.append(lax.ppermute(passed[s], "dp", across))

        whole = [None] * 3
        sources = [*gathered[:2], *onward[:2]]
        moves = [u for i in (0, 1) for u in known_moves(chunks, i, i, [2, 3], i)]
        whole[:2] = move(moves, sources, gathered[:2])
        sources = [gathered[2], *onward[2:-1], *moments]
        first = len(sources) - len(moments)
        moves = known_moves(chunks, 2, 0, [None, None, *range(1, first), None], 0)
        for a, array in enumerate(moments):
            for layer in range(array.shape[0]):
                for h in (0, 1):
                    at = lambda chip, core, layer=layer, h=h: (layer, h)
                    moves.append(Move(first + a, at, 1 + a, at, array.shape[2:]))
        whole[2], *moments = move(moves, sources, [gathered[2], *moments])

        for place, group in enumerate(([0], [1], [2], range(3, len(stages)))):
            which = stages[group[0]][0][0].which
            sources, moves = [], []
            for s in group:
                moves += last_moves(stages[s], (len(sources), len(sources) + 1), 0, joined=s == len(stages) - 1)
                sources += [passed[s], crossed[s]]
            if place == 2:
                moves += late_moves(stages[-1], (2, 3), 0)
                sources += late
            whole[which] = put(moves, sources, whole[which])
        return tuple(a.reshape(s) for a, s in zip((*whole, *moments), shapes[3:]))

    all_of, cut = P(None, None, None), P(None, "dp", None)
    return jax.shard_map(
        step,
        mesh=mesh,
        in_specs=(P(("rep", "dp"), None, None, None),) * 3 + (all_of,) * 3 + (cut,) * 6,
        out_specs=(P("rep", None, None),) * 3 + (P("rep", "dp", None),) * 6,
        check_vma=False,
    )
```

```python
import functools

import jax
import jax.numpy as jnp
from jax import lax
from jax.experimental import pallas as pl
from jax.experimental.pallas import tpu as pltpu
from jax.sharding import PartitionSpec as P


MESH = pl.DeviceIdType.MESH
F32, BF16 = jnp.float32, jnp.bfloat16
VMEM_LIMIT = 63 * 2**20
CHIPS = 4
OPPOSITE, RIGHT, LEFT, OWN = range(4)
OFFSET = (2, 1, 3, 0)
FIRST_ROWS = 16
LAST_ROWS = 56


def adamw(w, m, v, g):
    m = 0.9 * m + 0.1 * g
    v = 0.95 * v + 0.05 * g * g
    step = m * lax.rsqrt(v + 1e-8) + 0.1 * w
    return (w - 0.02 * step).astype(BF16), m, v


class Chunk:
    def __init__(self, number, which, layer, kind, place, rows, cols):
        self.number, self.which, self.layer = number, which, layer
        self.kind, self.place = kind, place
        self.rows, self.cols = rows, cols
        self.width = 640 if cols % 640 == 0 else 512
        self.segments = []


def plan(shapes):
    kinds, chunks, used = [], [], []
    for which, (layers, _, rows, cols) in enumerate(shapes):
        if (rows, cols) not in kinds:
            kinds.append((rows, cols))
            used.append(0)
        kind = kinds.index((rows, cols))
        for layer in range(layers):
            chunks.append(Chunk(len(chunks), which, layer, kind, used[kind], rows, cols))
            used[kind] += 1
    stages, count = [], 0
    for c in chunks:
        last = c.which == chunks[-1].which
        cuts = [0, c.rows - LAST_ROWS, c.rows] if c is chunks[-1] else [0, c.rows]
        for start, stop in zip(cuts, cuts[1:]):
            if last or not stages or stages[-1][0][0].which != c.which:
                stages.append([])
            stages[-1].append((c, start, stop - start))
            c.segments.append((count, len(stages) - 1, len(stages[-1]) - 1, start, stop - start))
            count += 1
    return chunks, kinds, used, stages, count


def exchange(chunks, kinds, used, stages, *refs):
    it = iter(refs)
    take = lambda n: [next(it) for _ in range(n)]
    g, w, m, v = take(3), take(3), take(3), take(3)
    out, new_m, new_v = take(3), take(3), take(3)
    to_go_right, to_go_left, *onward = take(len(stages) + 1)
    onward = [None, *onward]
    nk = len(kinds)
    peer, pass_in, near_in, own, w_in, m_in, v_in = (take(nk) for _ in range(7))
    (first_in, lead_sem, first_sem, lead_send, x_send, x_recv, a_send, a_recv, b_send, b_recv, own_sem, in_sem, out_sem, kept_sem, g_send, g_recv,
     gx_send, gx_recv) = it
    n = len(chunks)

    me = lax.axis_index("dp")
    chip, core = me // 2, me % 2
    right = lax.rem(chip + 1, CHIPS) * 2 + core
    left = lax.rem(chip + CHIPS - 1, CHIPS) * 2 + core
    other = chip * 2 + (1 - core)
    chip_at = [lax.rem(chip + OFFSET[r], CHIPS) for r in range(4)]
    ahead_chip, behind_chip = (lax.rem(chip + 1 + 2 * (core if s else 1 - core), CHIPS) for s in (1, 0))
    ahead, behind = ahead_chip * 2 + core, behind_chip * 2 + core

    barrier = pltpu.get_barrier_semaphore()
    for d in (right, left, other):
        pl.semaphore_signal(barrier, inc=1, device_id={"dp": d}, device_id_type=MESH)

    def remote(src, dst, send, recv, to):
        pltpu.make_async_remote_copy(
            src_ref=src, dst_ref=dst, send_sem=send, recv_sem=recv, device_id={"dp": to}, device_id_type=MESH).start()

    def await_bytes(ref, sem):
        pltpu.make_async_copy(ref, ref, sem).wait()

    order = [(OPPOSITE, c) for c in chunks]
    for c in chunks:
        order += [(RIGHT, c), (LEFT, c)]
    order += [(OWN, c) for c in chunks]
    slots, seen = {}, [0] * nk
    for r, c in order:
        slots[r, c.number] = seen[c.kind] % 3
        seen[c.kind] += 1

    def own_load(p):
        r, c = order[p]
        slot = slots[r, c.number]
        return pltpu.make_async_copy(
            g[c.which].at[c.layer, pl.ds((chip_at[r] * 2 + core) * 2, 2)], own[c.kind].at[slot], own_sem.at[c.kind * 3 + slot])

    def load_state(c):
        s = c.place % 2
        sem = (c.kind * 2 + s) * 2
        pltpu.make_async_copy(w[c.which].at[c.layer, pl.ds(me * 2, 2)], w_in[c.kind].at[s], in_sem.at[sem]).start()
        pltpu.make_async_copy(m[c.which].at[c.layer], m_in[c.kind].at[s], in_sem.at[sem + 1]).start()
        pltpu.make_async_copy(v[c.which].at[c.layer], v_in[c.kind].at[s], in_sem.at[sem + 1]).start()

    first = chunks[0]
    pieces = [(h, rows) for rows in ((0, FIRST_ROWS), (FIRST_ROWS, first.rows)) for h in (0, 1)]

    def given(h, start, stop):
        return g[first.which].at[first.layer, (chip_at[OPPOSITE] * 2 + (1 - core)) * 2 + h, pl.ds(start, stop - start)]

    for h in (0, 1):
        pltpu.make_async_copy(given(h, 0, FIRST_ROWS), first_in.at[h], first_sem.at[0]).start()
    own_load(0).start()
    own_load(1).start()
    await_bytes(first_in, first_sem.at[0])
    pl.semaphore_wait(barrier, 3)

    def swap(r, c):
        remote(
            g[c.which].at[c.layer, pl.ds((chip_at[r] * 2 + (1 - core)) * 2, 2)], peer[c.kind].at[r, c.place],
            x_send.at[c.kind], x_recv.at[{OPPOSITE: 0, RIGHT: n, LEFT: n, OWN: 2 * n}[r] + c.number], other)

    def first_piece(h, start, stop):
        return peer[first.kind].at[OPPOSITE, first.place, h, pl.ds(start, stop - start)]

    for k, (h, (start, stop)) in enumerate(pieces):
        remote(
            first_in.at[h] if start == 0 else given(h, start, stop), first_piece(h, start, stop),
            x_send.at[first.kind], x_recv.at[3 * n + k], other)
    for c in chunks[1:]:
        swap(OPPOSITE, c)

    position = [0]

    def take_own(r, c):
        p = position[0]
        position[0] += 1
        assert order[p] == (r, c)
        if p + 2 < len(order):
            own_load(p + 2).start()
        own_load(p).wait()
        if r == RIGHT:
            await_bytes(peer[c.kind].at[pl.ds(RIGHT, 2), c.place], x_recv.at[n + c.number])
        elif r == OWN or r == OPPOSITE and c is not first:
            await_bytes(peer[c.kind].at[r, c.place], x_recv.at[(0 if r == OPPOSITE else 2 * n) + c.number])
        return own[c.kind].at[slots[r, c.number]], peer[c.kind].at[r, c.place]

    def tiles(c, start, stop, body):
        whole = (stop - start) // 16
        cols = [pl.ds(k, c.width) for k in range(0, c.cols, c.width)]

        @pl.loop(0, whole)
        def _(t):
            for k in cols:
                body(pl.ds(pl.multiple_of(start + t * 16, 16), 16), k)

        if start + whole * 16 < stop:
            for k in cols:
                body(pl.ds(start + whole * 16, stop - start - whole * 16), k)

    def add(c, h, mine, theirs, *more, rows=None):
        def tile(r, k):
            total = mine[h, r, k].astype(F32) + theirs[h, r, k].astype(F32)
            for ref in more:
                total += ref[h, r, k].astype(F32)
            theirs[h, r, k] = total.astype(BF16)

        tiles(c, *(rows or (0, c.rows)), tile)

    for c in chunks:
        mine, theirs = take_own(OPPOSITE, c)
        for k, (h, (start, stop)) in enumerate(pieces if c is first else [(0, (0, c.rows)), (1, (0, c.rows))]):
            if c is first:
                await_bytes(first_piece(h, start, stop), x_recv.at[3 * n + k])
            add(c, h, mine, theirs, rows=(start, stop))
            if c is first and k == 0:

                @pl.when(core == 1)
                def _():
                    pl.semaphore_wait(lead_sem, 1)

            remote(
                theirs.at[h, pl.ds(start, stop - start)], pass_in[c.kind].at[c.place, h, pl.ds(start, stop - start)],
                lead_send.at[0] if c is first else a_send.at[c.kind], a_recv.at[c.number], (right, left)[h])
        swap(RIGHT, c)
        swap(LEFT, c)
        if c.number == 1:

            @pl.when(core == 0)
            def _():
                await_bytes(pass_in[first.kind].at[first.place], lead_send.at[0])
                pl.semaphore_signal(lead_sem, inc=1, device_id={"dp": other}, device_id_type=MESH)

    for c in chunks:
        for r, to, side in ((RIGHT, right, 0), (LEFT, left, 1)):
            mine, theirs = take_own(r, c)
            if r == RIGHT:
                await_bytes(pass_in[c.kind].at[c.place], a_recv.at[c.number])
            for h in (side, 1 - side):
                add(c, h, mine, theirs, *([pass_in[c.kind].at[c.place]] if h == side else []))
                remote(theirs.at[h], near_in[c.kind].at[side, c.place, h], b_send.at[c.kind], b_recv.at[c.number], to)
        swap(OWN, c)

    for c in chunks[:2]:
        load_state(c)
    storing = []

    def await_moments(c):
        await_bytes(m_in[c.kind], out_sem.at[c.kind * 2 + c.place % 2])

    for c in chunks:
        mine, theirs = take_own(OWN, c)
        s = c.place % 2
        await_bytes(w_in[c.kind].at[s], in_sem.at[(c.kind * 2 + s) * 2])
        await_bytes(m_in[c.kind], in_sem.at[(c.kind * 2 + s) * 2 + 1])
        await_bytes(near_in[c.kind].at[:, c.place], b_recv.at[c.number])
        from_left, from_right = near_in[c.kind].at[0, c.place], near_in[c.kind].at[1, c.place]
        w_ref, m_ref, v_ref = w_in[c.kind].at[s], m_in[c.kind].at[s], v_in[c.kind].at[s]
        for h in (0, 1):

            def tile(r, k):
                total = mine[h, r, k].astype(F32) + theirs[h, r, k].astype(F32)
                total += from_left[h, r, k].astype(F32) + from_right[h, r, k].astype(F32)
                gradient = total.astype(BF16).astype(F32)
                new = adamw(w_ref[h, r, k].astype(F32), m_ref[h, r, k], v_ref[h, r, k], gradient)
                theirs[h, r, k], m_ref[h, r, k], v_ref[h, r, k] = new

            tiles(c, 0, c.rows, tile)
        for number, stage, index, start, size in c.segments:
            rows = pl.ds(start, size)
            here = lambda h: out[c.which].at[c.layer, me * 2 + h, rows]
            if stage == 0:
                sends = (
                    (0, right, to_go_right.at[index]), (1, right, here(1)), (1, left, to_go_left.at[index]), (0, left, here(0)))
            elif c is chunks[-1]:
                e = onward[stage]
                sends = (
                    (core, ahead, e.at[0]), (1 - core, ahead, e.at[1]), (1 - core, behind, e.at[2]), (core, behind, e.at[3]))
            else:
                sends = (
                    (core, ahead, onward[stage].at[index, core]), (1 - core, ahead, here(1 - core)),
                    (1 - core, behind, here(1 - core)), (core, behind, here(core)))
            for h, to, dst in sends:
                remote(theirs.at[h, rows], dst, g_send.at[c.kind], g_recv.at[number], to)
        target = out[c.which].at[c.layer, pl.ds(me * 2, 2)]
        remote(theirs, target, gx_send.at[c.kind], gx_recv.at[c.kind], other)
        pltpu.make_async_copy(theirs, target, kept_sem.at[c.kind]).start()
        pltpu.make_async_copy(m_ref, new_m[c.which].at[c.layer], out_sem.at[c.kind * 2 + s]).start()
        pltpu.make_async_copy(v_ref, new_v[c.which].at[c.layer], out_sem.at[c.kind * 2 + s]).start()
        storing.append(c)
        if 1 <= c.number < n - 1:
            following = chunks[c.number + 1]
            for before in storing[:-1]:
                if before.kind == following.kind and before.place == following.place - 2:
                    await_moments(before)
                    storing.remove(before)
            load_state(following)

    full = [sum(c.kind == kind for c in chunks[:-1]) for kind in range(nk)]
    for c in chunks:
        for number, stage, index, start, size in c.segments:
            rows = pl.ds(start, size)
            await_bytes(near_in[c.kind].at[:, c.place, :, rows], g_recv.at[number])
            if c is chunks[-1]:
                continue
            there = lambda owner, h: out[c.which].at[c.layer, (owner * 2 + core) * 2 + h]
            if stage == 0:
                moves = (
                    (to_go_right.at[index], there(chip_at[LEFT], 0)), (there(chip_at[LEFT], 1),) * 2,
                    (to_go_left.at[index], there(chip_at[RIGHT], 1)), (there(chip_at[RIGHT], 0),) * 2)
            else:
                mine = onward[stage].at[index, core]
                moves = (
                    (mine, there(behind_chip, core)), (there(behind_chip, 1 - core),) * 2,
                    (there(ahead_chip, 1 - core), mine), (there(ahead_chip, core),) * 2)
            for src, dst in moves:
                remote(src, dst, gx_send.at[nk + c.kind], gx_recv.at[nk + c.kind], other)
    for c in storing:
        await_moments(c)
    for kind in range(nk):
        await_bytes(peer[kind], x_send.at[kind])
        if kind == first.kind:
            await_bytes(pass_in[kind].at[pl.ds(1, used[kind] - 1)], a_send.at[kind])
        else:
            await_bytes(pass_in[kind], a_send.at[kind])
        await_bytes(peer[kind].at[pl.ds(1, 2)], b_send.at[kind])
        await_bytes(peer[kind].at[pl.ds(0, 2)], g_send.at[kind])
        await_bytes(peer[kind].at[0], gx_send.at[kind])
        await_bytes(peer[kind].at[0], gx_recv.at[kind])
        await_bytes(peer[kind].at[0], kept_sem.at[kind])
        if full[kind]:
            await_bytes(near_in[kind].at[:, pl.ds(0, full[kind])], gx_send.at[nk + kind])
            await_bytes(near_in[kind].at[:, pl.ds(0, full[kind])], gx_recv.at[nk + kind])

    @pl.when(core == 1)
    def _():
        await_bytes(pass_in[first.kind].at[first.place], lead_send.at[0])


def gather_step(chunks, kinds, used, stages, segments, terms, weights, m, v):
    n, nk = len(chunks), len(kinds)
    hbm = pl.BlockSpec(memory_space=pltpu.HBM)
    slots = lambda lead, dtype: [
        pltpu.VMEM((*(u if x is None else x for x in lead), 2, *k), dtype) for k, u in zip(kinds, used)]
    dma = lambda count: pltpu.SemaphoreType.DMA((count,))
    results = [jax.ShapeDtypeStruct(w.shape, BF16) for w in weights]
    results += [jax.ShapeDtypeStruct(a.shape, F32) for a in (*m, *v)]
    results += [jax.ShapeDtypeStruct((len(stages[0]), *kinds[stages[0][0][0].kind]), BF16)] * 2
    for s in stages[1:]:
        lead = (4,) if s[0][0] is chunks[-1] else (len(s), 2)
        results.append(jax.ShapeDtypeStruct((*lead, s[0][2], s[0][0].cols), BF16))
    return pl.pallas_call(
        functools.partial(exchange, chunks, kinds, used, stages),
        out_shape=results,
        in_specs=[hbm] * 12,
        out_specs=[hbm] * len(results),
        scratch_shapes=[
            *slots((4, None), BF16), *slots((None,), BF16), *slots((2, None), BF16), *slots((3,), BF16),
            *slots((2,), BF16), *slots((2,), F32), *slots((2,), F32),
            pltpu.VMEM((2, FIRST_ROWS, chunks[0].cols), BF16), pltpu.SemaphoreType.REGULAR, dma(1), dma(1),
            dma(nk), dma(3 * n + 4), dma(nk), dma(n), dma(nk), dma(n), dma(3 * nk), dma(4 * nk), dma(2 * nk), dma(nk),
            dma(nk), dma(segments), dma(2 * nk), dma(2 * nk),
        ],
        compiler_params=pltpu.CompilerParams(collective_id=0, has_side_effects=True, vmem_limit_bytes=VMEM_LIMIT),
    )(*terms, *weights, *m, *v)


class Move:
    def __init__(self, source, source_at, target, target_at, shape):
        self.source, self.source_at = source, source_at
        self.target, self.target_at = target, target_at
        self.shape = shape


def move_body(moves, kinds, depth, n_in, n_out, *refs):
    sources, targets = refs[:n_in], refs[n_in : n_in + n_out]
    bufs, (in_sem, out_sem) = refs[n_in + n_out : -2], refs[-2:]
    me = lax.axis_index("dp")
    chip, core = me // 2, me % 2
    seen, place = [0] * len(kinds), []
    for u in moves:
        place.append((u.kind, seen[u.kind] % depth[u.kind]))
        seen[u.kind] += 1
    sem = {slot: k for k, slot in enumerate(sorted(set(place)))}

    def load(i):
        u, (kind, slot) = moves[i], place[i]
        return pltpu.make_async_copy(
            sources[u.source].at[u.source_at(chip, core)], bufs[kind].at[slot], in_sem.at[sem[place[i]]])

    def store(i):
        u, (kind, slot) = moves[i], place[i]
        return pltpu.make_async_copy(
            bufs[kind].at[slot], targets[u.target].at[u.target_at(chip, core)], out_sem.at[sem[place[i]]])

    waited, last = set(), {}

    def start(i):
        if place[i] in last:
            store(last[place[i]]).wait()
            waited.add(last[place[i]])
        last[place[i]] = i
        load(i).start()

    ahead = 8
    for i in range(min(ahead, len(moves))):
        start(i)
    for i in range(len(moves)):
        load(i).wait()
        store(i).start()
        if i + ahead < len(moves):
            start(i + ahead)
    for i in range(len(moves)):
        if i not in waited:
            store(i).wait()


def move(moves, sources, targets):
    kinds, counts = [], []
    for u in moves:
        kind = (u.shape, sources[u.source].dtype)
        if kind not in kinds:
            kinds.append(kind)
            counts.append(0)
        u.kind = kinds.index(kind)
        counts[u.kind] += 1
    depth = [min(12, c) for c in counts]
    size = lambda shape: functools.reduce(lambda a, b: a * b, shape)
    nbytes = 2 * sum(size(shape) * dtype.itemsize * c for (shape, dtype), c in zip(kinds, counts))
    hbm = pl.BlockSpec(memory_space=pltpu.HBM)
    return pl.pallas_call(
        functools.partial(move_body, moves, kinds, depth, len(sources), len(targets)),
        out_shape=[jax.ShapeDtypeStruct(a.shape, a.dtype) for a in targets],
        in_specs=[hbm] * len(sources),
        out_specs=[hbm] * len(targets),
        scratch_shapes=[pltpu.VMEM((d, *shape), dtype) for d, (shape, dtype) in zip(depth, kinds)]
        + [pltpu.SemaphoreType.DMA((sum(depth),)), pltpu.SemaphoreType.DMA((sum(depth),))],
        compiler_params=pltpu.CompilerParams(vmem_limit_bytes=56 * 2**20),
        cost_estimate=pl.CostEstimate(flops=2 * nbytes, bytes_accessed=nbytes, transcendentals=0),
    )(*sources)


def put_body(moves, n_in, *refs):
    sources, target, sem = refs[:n_in], refs[-2], refs[-1]
    me = lax.axis_index("dp")
    chip, core = me // 2, me % 2
    copies = [
        pltpu.make_async_copy(
            sources[u.source].at[u.source_at(chip, core)], target.at[u.target_at(chip, core)], sem.at[i])
        for i, u in enumerate(moves)
    ]
    for copy in copies:
        copy.start()
    for copy in copies:
        copy.wait()


def put(moves, sources, into):
    nbytes = 2 * sum(a.size * a.dtype.itemsize for a in sources)
    hbm = pl.BlockSpec(memory_space=pltpu.HBM)
    return pl.pallas_call(
        functools.partial(put_body, moves, len(sources) + 1),
        out_shape=jax.ShapeDtypeStruct(into.shape, into.dtype),
        in_specs=[pl.BlockSpec(memory_space=pltpu.VMEM)] * len(sources) + [hbm],
        out_specs=hbm,
        input_output_aliases={len(sources): 0},
        scratch_shapes=[pltpu.SemaphoreType.DMA((len(moves),))],
        compiler_params=pltpu.CompilerParams(vmem_limit_bytes=16 * 2**20),
        cost_estimate=pl.CostEstimate(flops=2 * nbytes, bytes_accessed=nbytes, transcendentals=0),
    )(*sources, into)


def known_moves(chunks, which, source, onward, target):
    def blocks(c, steps, block):
        return lambda chip, core: (c.layer, pl.ds((lax.rem(chip + steps * (1 + 2 * core), CHIPS) * 2 + block(core)) * 2, 2))

    def behind(c, parity, h):
        return lambda chip, core: (c.layer, (lax.rem(chip + 3 - 2 * core, CHIPS) * 2 + parity) * 2 + h(core))

    def beside(c, r, h):
        return lambda chip, core: (c.layer, (lax.rem(chip + OFFSET[r], CHIPS) * 2 + core) * 2 + h)

    def at(*index):
        return lambda chip, core: index

    def add(source, source_at, place, shape):
        moves.append(Move(source, source_at, target, place, shape))

    mine, its, moves = (lambda core: core), (lambda core: 1 - core), []
    for c in (c for c in chunks if c.which == which):
        block, piece = (2, c.rows, c.cols), (c.rows, c.cols)
        for place in (blocks(c, 0, mine), blocks(c, 0, its)):
            add(source, place, place, block)
        if c is chunks[-1]:
            continue
        ((_, stage, index, _, _),) = c.segments
        if stage == 0:
            for steps in (1, 3):
                place = blocks(c, steps, its)
                add(source, place, place, block)
            for passed, r in enumerate((LEFT, RIGHT)):
                add(onward[0][passed], at(index), beside(c, r, passed), piece)
                place = beside(c, r, 1 - passed)
                add(source, place, place, piece)
        else:
            for parity in (0, 1):
                place = blocks(c, 1, lambda core, parity=parity: parity)
                add(source, place, place, block)
                place = behind(c, parity, its)
                add(source, place, place, piece)
                add(onward[stage], at(index, parity), behind(c, parity, mine), piece)
    return moves


def late_moves(stage, sources, target):
    (c, start, size), moves = stage[0], []
    for k, source in enumerate(sources):
        for i in range(4):
            def to(chip, core, k=k, i=i):
                there = core if k == 0 else 1 - core
                owner = lax.rem(chip + (3 - 2 * there if i < 2 else 1 + 2 * there), CHIPS) * 2 + there
                return c.layer, owner * 2 + (there if i in (0, 3) else 1 - there), pl.ds(start, size)

            moves.append(Move(source, lambda chip, core, i=i: (i,), target, to, (size, c.cols)))
    return moves


def first_moves(stage, sources, target):
    moves = []
    for index, (c, _, _) in enumerate(stage):
        for k, source in enumerate(sources):
            def to(chip, core, c=c, k=k):
                owner = lax.rem(chip + 2, CHIPS) * 2 + (core if k < 2 else 1 - core)
                return c.layer, owner * 2 + k % 2

            moves.append(Move(source, lambda chip, core, index=index: (index,), target, to, (c.rows, c.cols)))
    return moves


def last_moves(stage, sources, target, joined=False):
    moves = []
    for index, (c, start, size) in enumerate(stage):
        for k, source in enumerate(sources):
            for parity in (0, 1):
                def to(chip, core, c=c, start=start, size=size, k=k, parity=parity):
                    half = core if k == 0 else 1 - core
                    owner = lax.rem(chip + 2, CHIPS) * 2 + ((half if parity == 0 else 1 - half) if joined else parity)
                    return c.layer, owner * 2 + half, pl.ds(start, size)

                at = lambda chip, core, index=index, parity=parity: (index, parity)
                moves.append(Move(source, at, target, to, (size, c.cols)))
    return moves


def solution(mesh):
    devices = mesh.shape["dp"]
    assert devices == 2 * CHIPS
    onward_to = [(d, (d + 2 - 4 * (d % 2)) % devices) for d in range(devices)]
    across = [(d, d ^ 1) for d in range(devices)]
    to_right = [(d, (d + 2) % devices) for d in range(devices)]
    to_left = [(d, (d - 2) % devices) for d in range(devices)]

    def halves(a, count):
        return a.reshape(a.shape[0], count, a.shape[1] // count, a.shape[2])

    def step(*arrays):
        shapes = [a.shape for a in arrays]
        terms = [halves(t[0], 2 * devices) for t in arrays[:3]]
        weights = [halves(w, 2 * devices) for w in arrays[3:6]]
        m, v = ([halves(a, 2) for a in arrays[i : i + 3]] for i in (6, 9))
        chunks, kinds, used, stages, segments = plan([w.shape for w in weights])
        results = gather_step(chunks, kinds, used, stages, segments, terms, weights, m, v)
        gathered, moments, first_stage, onward = results[:3], results[3:9], results[9:11], list(results[11:])
        late = range(len(stages) - len(chunks[-1].segments), len(stages))

        passed, crossed = {}, {}

        def hop(s, piece, to):
            passed.setdefault(s, []).append(lax.ppermute(piece, "dp", to))
            crossed.setdefault(s, []).append(lax.ppermute(passed[s][-1], "dp", across))

        hop(0, first_stage[0], to_right)
        hop(0, first_stage[1], to_left)
        onward = dict(enumerate(onward, 1))
        for s in range(1, late.start):
            hop(s, onward[s], onward_to)
        after = {s: lax.ppermute(onward[s], "dp", across) for s in late}
        for s in late:
            hop(s, jnp.stack([onward[s][0], after[s][2]])[None], onward_to)

        whole = [None] * 3
        sources = [*gathered[:2], *first_stage, onward[1]]
        moves = [u for i in (0, 1) for u in known_moves(chunks, i, i, [(2, 3), 4], i)]
        whole[:2] = move(moves, sources, gathered[:2])
        sources = [gathered[2], onward[2], *moments]
        moves = known_moves(chunks, 2, 0, [None, None, 1], 0)
        for a, array in enumerate(moments):
            for layer in range(array.shape[0]):
                for h in (0, 1):
                    at = lambda chip, core, layer=layer, h=h: (layer, h)
                    moves.append(Move(2 + a, at, 1 + a, at, array.shape[2:]))
        whole[2], *moments = move(moves, sources, [gathered[2], *moments])

        whole[0] = put(first_moves(stages[0], range(4), 0), [*passed[0], *crossed[0]], whole[0])
        for place, group in enumerate(([1], [2], late), 1):
            which = stages[group[0]][0][0].which
            sources, moves = [], []
            for s in group:
                moves += last_moves(stages[s], (len(sources), len(sources) + 1), 0, joined=s in late)
                sources += [*passed[s], *crossed[s]]
            if place == 2:
                for s in late:
                    moves += late_moves(stages[s], (len(sources), len(sources) + 1), 0)
                    sources += [onward[s], after[s]]
            whole[which] = put(moves, sources, whole[which])
        return tuple(a.reshape(s) for a, s in zip((*whole, *moments), shapes[3:]))

    all_of, cut = P(None, None, None), P(None, "dp", None)
    return jax.shard_map(
        step,
        mesh=mesh,
        in_specs=(P(("rep", "dp"), None, None, None),) * 3 + (all_of,) * 3 + (cut,) * 6,
        out_specs=(P("rep", None, None),) * 3 + (P("rep", "dp", None),) * 6,
        check_vma=False,
    )
```

```python
import functools

import jax
import jax.numpy as jnp
from jax import lax
from jax.experimental import pallas as pl
from jax.experimental.pallas import tpu as pltpu
from jax.sharding import PartitionSpec as P


MESH = pl.DeviceIdType.MESH
F32, BF16 = jnp.float32, jnp.bfloat16
VMEM_LIMIT = 63 * 2**20
CHIPS = 4
OPPOSITE, RIGHT, LEFT, OWN = range(4)
OFFSET = (2, 1, 3, 0)
FIRST_ROWS = 16
LAST_ROWS = 56


def adamw(w, m, v, g):
    m = 0.9 * m + 0.1 * g
    v = 0.95 * v + 0.05 * g * g
    step = m * lax.rsqrt(v + 1e-8) + 0.1 * w
    return (w - 0.02 * step).astype(BF16), m, v


class Chunk:
    def __init__(self, number, which, layer, kind, place, rows, cols):
        self.number, self.which, self.layer = number, which, layer
        self.kind, self.place = kind, place
        self.rows, self.cols = rows, cols
        self.width = 640 if cols % 640 == 0 else 512
        self.segments = []


def plan(shapes):
    kinds, chunks, used = [], [], []
    for which, (layers, _, rows, cols) in enumerate(shapes):
        if (rows, cols) not in kinds:
            kinds.append((rows, cols))
            used.append(0)
        kind = kinds.index((rows, cols))
        for layer in range(layers):
            chunks.append(Chunk(len(chunks), which, layer, kind, used[kind], rows, cols))
            used[kind] += 1
    stages, count = [], 0
    for c in chunks:
        last = c.which == chunks[-1].which
        cuts = [0, c.rows - LAST_ROWS, c.rows] if c is chunks[-1] else [0, c.rows]
        for start, stop in zip(cuts, cuts[1:]):
            if last or not stages or stages[-1][0][0].which != c.which:
                stages.append([])
            stages[-1].append((c, start, stop - start))
            c.segments.append((count, len(stages) - 1, len(stages[-1]) - 1, start, stop - start))
            count += 1
    return chunks, kinds, used, stages, count


def exchange(chunks, kinds, used, stages, *refs):
    it = iter(refs)
    take = lambda n: [next(it) for _ in range(n)]
    g, w, m, v = take(3), take(3), take(3), take(3)
    out, new_m, new_v = take(3), take(3), take(3)
    to_go_right, to_go_left, *onward = take(len(stages) + 1)
    onward = [None, *onward]
    nk = len(kinds)
    peer, pass_in, near_in, own, w_in, m_in, v_in = (take(nk) for _ in range(7))
    (first_in, lead_sem, first_sem, lead_send, x_send, x_recv, a_send, a_recv, b_send, b_recv, own_sem, in_sem, out_sem, kept_sem, g_send, g_recv,
     gx_send, gx_recv) = it
    n = len(chunks)

    me = lax.axis_index("dp")
    chip, core = me // 2, me % 2
    right = lax.rem(chip + 1, CHIPS) * 2 + core
    left = lax.rem(chip + CHIPS - 1, CHIPS) * 2 + core
    other = chip * 2 + (1 - core)
    chip_at = [lax.rem(chip + OFFSET[r], CHIPS) for r in range(4)]
    ahead_chip, behind_chip = (lax.rem(chip + 1 + 2 * (core if s else 1 - core), CHIPS) for s in (1, 0))
    ahead, behind = ahead_chip * 2 + core, behind_chip * 2 + core

    barrier = pltpu.get_barrier_semaphore()
    for d in (right, left, other):
        pl.semaphore_signal(barrier, inc=1, device_id={"dp": d}, device_id_type=MESH)

    def remote(src, dst, send, recv, to):
        pltpu.make_async_remote_copy(
            src_ref=src, dst_ref=dst, send_sem=send, recv_sem=recv, device_id={"dp": to}, device_id_type=MESH).start()

    def await_bytes(ref, sem):
        pltpu.make_async_copy(ref, ref, sem).wait()

    order = [(OPPOSITE, c) for c in chunks]
    for c in chunks:
        order += [(RIGHT, c), (LEFT, c)]
    order += [(OWN, c) for c in chunks]
    slots, seen = {}, [0] * nk
    for r, c in order:
        slots[r, c.number] = seen[c.kind] % 3
        seen[c.kind] += 1

    def own_load(p):
        r, c = order[p]
        slot = slots[r, c.number]
        return pltpu.make_async_copy(
            g[c.which].at[c.layer, pl.ds((chip_at[r] * 2 + core) * 2, 2)], own[c.kind].at[slot], own_sem.at[c.kind * 3 + slot])

    def load_state(c):
        s = c.place % 2
        sem = (c.kind * 2 + s) * 2
        pltpu.make_async_copy(w[c.which].at[c.layer, pl.ds(me * 2, 2)], w_in[c.kind].at[s], in_sem.at[sem]).start()
        pltpu.make_async_copy(m[c.which].at[c.layer], m_in[c.kind].at[s], in_sem.at[sem + 1]).start()
        pltpu.make_async_copy(v[c.which].at[c.layer], v_in[c.kind].at[s], in_sem.at[sem + 1]).start()

    first = chunks[0]
    pieces = [(h, rows) for rows in ((0, FIRST_ROWS), (FIRST_ROWS, first.rows)) for h in (0, 1)]

    def given(h, start, stop):
        return g[first.which].at[first.layer, (chip_at[OPPOSITE] * 2 + (1 - core)) * 2 + h, pl.ds(start, stop - start)]

    for h in (0, 1):
        pltpu.make_async_copy(given(h, 0, FIRST_ROWS), first_in.at[h], first_sem.at[0]).start()
    own_load(0).start()
    own_load(1).start()
    await_bytes(first_in, first_sem.at[0])
    pl.semaphore_wait(barrier, 3)

    def swap(r, c):
        remote(
            g[c.which].at[c.layer, pl.ds((chip_at[r] * 2 + (1 - core)) * 2, 2)], peer[c.kind].at[r, c.place],
            x_send.at[c.kind], x_recv.at[{OPPOSITE: 0, RIGHT: n, LEFT: n, OWN: 2 * n}[r] + c.number], other)

    def first_piece(h, start, stop):
        return peer[first.kind].at[OPPOSITE, first.place, h, pl.ds(start, stop - start)]

    for k, (h, (start, stop)) in enumerate(pieces):
        remote(
            first_in.at[h] if start == 0 else given(h, start, stop), first_piece(h, start, stop),
            x_send.at[first.kind], x_recv.at[3 * n + k], other)
    for c in chunks[1:]:
        swap(OPPOSITE, c)

    position = [0]

    def take_own(r, c):
        p = position[0]
        position[0] += 1
        assert order[p] == (r, c)
        if p + 2 < len(order):
            own_load(p + 2).start()
        own_load(p).wait()
        if r == RIGHT:
            await_bytes(peer[c.kind].at[pl.ds(RIGHT, 2), c.place], x_recv.at[n + c.number])
        elif r == OWN or r == OPPOSITE and c is not first:
            await_bytes(peer[c.kind].at[r, c.place], x_recv.at[(0 if r == OPPOSITE else 2 * n) + c.number])
        return own[c.kind].at[slots[r, c.number]], peer[c.kind].at[r, c.place]

    def tiles(c, start, stop, body):
        whole = (stop - start) // 16
        cols = [pl.ds(k, c.width) for k in range(0, c.cols, c.width)]

        @pl.loop(0, whole)
        def _(t):
            for k in cols:
                body(pl.ds(pl.multiple_of(start + t * 16, 16), 16), k)

        if start + whole * 16 < stop:
            for k in cols:
                body(pl.ds(start + whole * 16, stop - start - whole * 16), k)

    def add(c, h, mine, theirs, *more, rows=None):
        def tile(r, k):
            total = mine[h, r, k].astype(F32) + theirs[h, r, k].astype(F32)
            for ref in more:
                total += ref[h, r, k].astype(F32)
            theirs[h, r, k] = total.astype(BF16)

        tiles(c, *(rows or (0, c.rows)), tile)

    for c in chunks:
        mine, theirs = take_own(OPPOSITE, c)
        for k, (h, (start, stop)) in enumerate(pieces if c is first else [(0, (0, c.rows)), (1, (0, c.rows))]):
            if c is first:
                await_bytes(first_piece(h, start, stop), x_recv.at[3 * n + k])
            add(c, h, mine, theirs, rows=(start, stop))
            if c is first and k == 0:

                @pl.when(core == 1)
                def _():
                    pl.semaphore_wait(lead_sem, 1)

            remote(
                theirs.at[h, pl.ds(start, stop - start)], pass_in[c.kind].at[c.place, h, pl.ds(start, stop - start)],
                lead_send.at[0] if c is first else a_send.at[c.kind], a_recv.at[c.number], (right, left)[h])
        swap(RIGHT, c)
        swap(LEFT, c)
        if c.number == 1:

            @pl.when(core == 0)
            def _():
                await_bytes(pass_in[first.kind].at[first.place], lead_send.at[0])
                pl.semaphore_signal(lead_sem, inc=1, device_id={"dp": other}, device_id_type=MESH)

    for c in chunks:
        for r, to, side in ((RIGHT, right, 0), (LEFT, left, 1)):
            mine, theirs = take_own(r, c)
            if r == RIGHT:
                await_bytes(pass_in[c.kind].at[c.place], a_recv.at[c.number])
            for h in (side, 1 - side):
                add(c, h, mine, theirs, *([pass_in[c.kind].at[c.place]] if h == side else []))
                remote(theirs.at[h], near_in[c.kind].at[side, c.place, h], b_send.at[c.kind], b_recv.at[c.number], to)
        swap(OWN, c)

    for c in chunks[:2]:
        load_state(c)
    storing = []

    def await_moments(c):
        await_bytes(m_in[c.kind], out_sem.at[c.kind * 2 + c.place % 2])

    for c in chunks:
        mine, theirs = take_own(OWN, c)
        s = c.place % 2
        await_bytes(w_in[c.kind].at[s], in_sem.at[(c.kind * 2 + s) * 2])
        await_bytes(m_in[c.kind], in_sem.at[(c.kind * 2 + s) * 2 + 1])
        await_bytes(near_in[c.kind].at[:, c.place], b_recv.at[c.number])
        from_left, from_right = near_in[c.kind].at[0, c.place], near_in[c.kind].at[1, c.place]
        w_ref, m_ref, v_ref = w_in[c.kind].at[s], m_in[c.kind].at[s], v_in[c.kind].at[s]
        for h in (0, 1):

            def tile(r, k):
                total = mine[h, r, k].astype(F32) + theirs[h, r, k].astype(F32)
                total += from_left[h, r, k].astype(F32) + from_right[h, r, k].astype(F32)
                gradient = total.astype(BF16).astype(F32)
                new = adamw(w_ref[h, r, k].astype(F32), m_ref[h, r, k], v_ref[h, r, k], gradient)
                theirs[h, r, k], m_ref[h, r, k], v_ref[h, r, k] = new

            tiles(c, 0, c.rows, tile)
        for number, stage, index, start, size in c.segments:
            rows = pl.ds(start, size)
            here = lambda h: out[c.which].at[c.layer, me * 2 + h, rows]
            if stage == 0:
                sends = (
                    (0, right, to_go_right.at[index]), (1, right, here(1)), (1, left, to_go_left.at[index]), (0, left, here(0)))
            elif c is chunks[-1]:
                e = onward[stage]
                sends = (
                    (core, ahead, e.at[0]), (1 - core, ahead, e.at[1]), (1 - core, behind, e.at[2]), (core, behind, e.at[3]))
            else:
                sends = (
                    (core, ahead, onward[stage].at[index, core]), (1 - core, ahead, here(1 - core)),
                    (1 - core, behind, here(1 - core)), (core, behind, here(core)))
            for h, to, dst in sends:
                remote(theirs.at[h, rows], dst, g_send.at[c.kind], g_recv.at[number], to)
        target = out[c.which].at[c.layer, pl.ds(me * 2, 2)]
        remote(theirs, target, gx_send.at[c.kind], gx_recv.at[c.kind], other)
        pltpu.make_async_copy(theirs, target, kept_sem.at[c.kind]).start()
        pltpu.make_async_copy(m_ref, new_m[c.which].at[c.layer], out_sem.at[c.kind * 2 + s]).start()
        pltpu.make_async_copy(v_ref, new_v[c.which].at[c.layer], out_sem.at[c.kind * 2 + s]).start()
        storing.append(c)
        if 1 <= c.number < n - 1:
            following = chunks[c.number + 1]
            for before in storing[:-1]:
                if before.kind == following.kind and before.place == following.place - 2:
                    await_moments(before)
                    storing.remove(before)
            load_state(following)

    full = [sum(c.kind == kind for c in chunks[:-1]) for kind in range(nk)]
    for c in chunks:
        for number, stage, index, start, size in c.segments:
            rows = pl.ds(start, size)
            await_bytes(near_in[c.kind].at[:, c.place, :, rows], g_recv.at[number])
            if c is chunks[-1]:
                continue
            there = lambda owner, h: out[c.which].at[c.layer, (owner * 2 + core) * 2 + h]
            if stage == 0:
                moves = (
                    (to_go_right.at[index], there(chip_at[LEFT], 0)), (there(chip_at[LEFT], 1),) * 2,
                    (to_go_left.at[index], there(chip_at[RIGHT], 1)), (there(chip_at[RIGHT], 0),) * 2)
            else:
                mine = onward[stage].at[index, core]
                moves = (
                    (mine, there(behind_chip, core)), (there(behind_chip, 1 - core),) * 2,
                    (there(ahead_chip, 1 - core), mine), (there(ahead_chip, core),) * 2)
            for src, dst in moves:
                remote(src, dst, gx_send.at[nk + c.kind], gx_recv.at[nk + c.kind], other)
    for c in storing:
        await_moments(c)
    for kind in range(nk):
        await_bytes(peer[kind], x_send.at[kind])
        if kind == first.kind:
            await_bytes(pass_in[kind].at[pl.ds(1, used[kind] - 1)], a_send.at[kind])
        else:
            await_bytes(pass_in[kind], a_send.at[kind])
        await_bytes(peer[kind].at[pl.ds(1, 2)], b_send.at[kind])
        await_bytes(peer[kind].at[pl.ds(0, 2)], g_send.at[kind])
        await_bytes(peer[kind].at[0], gx_send.at[kind])
        await_bytes(peer[kind].at[0], gx_recv.at[kind])
        await_bytes(peer[kind].at[0], kept_sem.at[kind])
        if full[kind]:
            await_bytes(near_in[kind].at[:, pl.ds(0, full[kind])], gx_send.at[nk + kind])
            await_bytes(near_in[kind].at[:, pl.ds(0, full[kind])], gx_recv.at[nk + kind])

    @pl.when(core == 1)
    def _():
        await_bytes(pass_in[first.kind].at[first.place], lead_send.at[0])


def gather_step(chunks, kinds, used, stages, segments, terms, weights, m, v):
    n, nk = len(chunks), len(kinds)
    hbm = pl.BlockSpec(memory_space=pltpu.HBM)
    slots = lambda lead, dtype: [
        pltpu.VMEM((*(u if x is None else x for x in lead), 2, *k), dtype) for k, u in zip(kinds, used)]
    dma = lambda count: pltpu.SemaphoreType.DMA((count,))
    results = [jax.ShapeDtypeStruct(w.shape, BF16) for w in weights]
    results += [jax.ShapeDtypeStruct(a.shape, F32) for a in (*m, *v)]
    results += [jax.ShapeDtypeStruct((len(stages[0]), *kinds[stages[0][0][0].kind]), BF16)] * 2
    for s in stages[1:]:
        lead = (4,) if s[0][0] is chunks[-1] else (len(s), 2)
        results.append(jax.ShapeDtypeStruct((*lead, s[0][2], s[0][0].cols), BF16))
    return pl.pallas_call(
        functools.partial(exchange, chunks, kinds, used, stages),
        out_shape=results,
        in_specs=[hbm] * 12,
        out_specs=[hbm] * len(results),
        scratch_shapes=[
            *slots((4, None), BF16), *slots((None,), BF16), *slots((2, None), BF16), *slots((3,), BF16),
            *slots((2,), BF16), *slots((2,), F32), *slots((2,), F32),
            pltpu.VMEM((2, FIRST_ROWS, chunks[0].cols), BF16), pltpu.SemaphoreType.REGULAR, dma(1), dma(1),
            dma(nk), dma(3 * n + 4), dma(nk), dma(n), dma(nk), dma(n), dma(3 * nk), dma(4 * nk), dma(2 * nk), dma(nk),
            dma(nk), dma(segments), dma(2 * nk), dma(2 * nk),
        ],
        compiler_params=pltpu.CompilerParams(collective_id=0, has_side_effects=True, vmem_limit_bytes=VMEM_LIMIT),
    )(*terms, *weights, *m, *v)


class Move:
    def __init__(self, source, source_at, target, target_at, shape):
        self.source, self.source_at = source, source_at
        self.target, self.target_at = target, target_at
        self.shape = shape


def move_body(moves, kinds, depth, n_in, n_out, *refs):
    sources, targets = refs[:n_in], refs[n_in : n_in + n_out]
    bufs, (in_sem, out_sem) = refs[n_in + n_out : -2], refs[-2:]
    me = lax.axis_index("dp")
    chip, core = me // 2, me % 2
    seen, place = [0] * len(kinds), []
    for u in moves:
        place.append((u.kind, seen[u.kind] % depth[u.kind]))
        seen[u.kind] += 1
    sem = {slot: k for k, slot in enumerate(sorted(set(place)))}

    def load(i):
        u, (kind, slot) = moves[i], place[i]
        return pltpu.make_async_copy(
            sources[u.source].at[u.source_at(chip, core)], bufs[kind].at[slot], in_sem.at[sem[place[i]]])

    def store(i):
        u, (kind, slot) = moves[i], place[i]
        return pltpu.make_async_copy(
            bufs[kind].at[slot], targets[u.target].at[u.target_at(chip, core)], out_sem.at[sem[place[i]]])

    waited, last = set(), {}

    def start(i):
        if place[i] in last:
            store(last[place[i]]).wait()
            waited.add(last[place[i]])
        last[place[i]] = i
        load(i).start()

    ahead = 8
    for i in range(min(ahead, len(moves))):
        start(i)
    for i in range(len(moves)):
        load(i).wait()
        store(i).start()
        if i + ahead < len(moves):
            start(i + ahead)
    for i in range(len(moves)):
        if i not in waited:
            store(i).wait()


def move(moves, sources, targets):
    kinds, counts = [], []
    for u in moves:
        kind = (u.shape, sources[u.source].dtype)
        if kind not in kinds:
            kinds.append(kind)
            counts.append(0)
        u.kind = kinds.index(kind)
        counts[u.kind] += 1
    depth = [min(12, c) for c in counts]
    size = lambda shape: functools.reduce(lambda a, b: a * b, shape)
    nbytes = 2 * sum(size(shape) * dtype.itemsize * c for (shape, dtype), c in zip(kinds, counts))
    hbm = pl.BlockSpec(memory_space=pltpu.HBM)
    return pl.pallas_call(
        functools.partial(move_body, moves, kinds, depth, len(sources), len(targets)),
        out_shape=[jax.ShapeDtypeStruct(a.shape, a.dtype) for a in targets],
        in_specs=[hbm] * len(sources),
        out_specs=[hbm] * len(targets),
        scratch_shapes=[pltpu.VMEM((d, *shape), dtype) for d, (shape, dtype) in zip(depth, kinds)]
        + [pltpu.SemaphoreType.DMA((sum(depth),)), pltpu.SemaphoreType.DMA((sum(depth),))],
        compiler_params=pltpu.CompilerParams(vmem_limit_bytes=56 * 2**20),
        cost_estimate=pl.CostEstimate(flops=2 * nbytes, bytes_accessed=nbytes, transcendentals=0),
    )(*sources)


def put_body(moves, n_in, *refs):
    sources, target, sem = refs[:n_in], refs[-2], refs[-1]
    me = lax.axis_index("dp")
    chip, core = me // 2, me % 2
    copies = [
        pltpu.make_async_copy(
            sources[u.source].at[u.source_at(chip, core)], target.at[u.target_at(chip, core)], sem.at[i])
        for i, u in enumerate(moves)
    ]
    for copy in copies:
        copy.start()
    for copy in copies:
        copy.wait()


def put(moves, sources, into):
    nbytes = 2 * sum(a.size * a.dtype.itemsize for a in sources)
    hbm = pl.BlockSpec(memory_space=pltpu.HBM)
    return pl.pallas_call(
        functools.partial(put_body, moves, len(sources) + 1),
        out_shape=jax.ShapeDtypeStruct(into.shape, into.dtype),
        in_specs=[pl.BlockSpec(memory_space=pltpu.VMEM)] * len(sources) + [hbm],
        out_specs=hbm,
        input_output_aliases={len(sources): 0},
        scratch_shapes=[pltpu.SemaphoreType.DMA((len(moves),))],
        compiler_params=pltpu.CompilerParams(vmem_limit_bytes=16 * 2**20),
        cost_estimate=pl.CostEstimate(flops=2 * nbytes, bytes_accessed=nbytes, transcendentals=0),
    )(*sources, into)


def fixed(*index):
    return lambda chip, core: index


def known_moves(chunks, which, source, onward, target):
    def blocks(c, steps, block):
        return lambda chip, core: (c.layer, pl.ds((lax.rem(chip + steps * (1 + 2 * core), CHIPS) * 2 + block(core)) * 2, 2))

    def behind(c, parity, h):
        return lambda chip, core: (c.layer, (lax.rem(chip + 3 - 2 * core, CHIPS) * 2 + parity) * 2 + h(core))

    def beside(c, r, h):
        return lambda chip, core: (c.layer, (lax.rem(chip + OFFSET[r], CHIPS) * 2 + core) * 2 + h)

    def add(source, source_at, place, shape):
        moves.append(Move(source, source_at, target, place, shape))

    mine, its, moves = (lambda core: core), (lambda core: 1 - core), []
    for c in (c for c in chunks if c.which == which):
        block, piece = (2, c.rows, c.cols), (c.rows, c.cols)
        for place in (blocks(c, 0, mine), blocks(c, 0, its)):
            add(source, place, place, block)
        if c is chunks[-1]:
            continue
        ((_, stage, index, _, _),) = c.segments
        if stage == 0:
            for steps in (1, 3):
                place = blocks(c, steps, its)
                add(source, place, place, block)
            for passed, r in enumerate((LEFT, RIGHT)):
                add(onward[0][passed], fixed(index), beside(c, r, passed), piece)
                place = beside(c, r, 1 - passed)
                add(source, place, place, piece)
        else:
            for parity in (0, 1):
                place = blocks(c, 1, lambda core, parity=parity: parity)
                add(source, place, place, block)
                place = behind(c, parity, its)
                add(source, place, place, piece)
                add(onward[stage], fixed(index, parity), behind(c, parity, mine), piece)
    return moves


def late_moves(stage, sources, target):
    (c, start, size), moves = stage[0], []
    for k, source in enumerate(sources):
        for i in range(4):
            def to(chip, core, k=k, i=i):
                there = core if k == 0 else 1 - core
                owner = lax.rem(chip + (3 - 2 * there if i < 2 else 1 + 2 * there), CHIPS) * 2 + there
                return c.layer, owner * 2 + (there if i in (0, 3) else 1 - there), pl.ds(start, size)

            moves.append(Move(source, fixed(i), target, to, (size, c.cols)))
    return moves


def first_moves(stage, sources, target):
    moves = []
    for index, (c, _, _) in enumerate(stage):
        for k, source in enumerate(sources):
            def to(chip, core, c=c, k=k):
                owner = lax.rem(chip + 2, CHIPS) * 2 + (core if k < 2 else 1 - core)
                return c.layer, owner * 2 + k % 2

            moves.append(Move(source, fixed(index), target, to, (c.rows, c.cols)))
    return moves


def last_moves(stage, sources, target, joined=False):
    moves = []
    for index, (c, start, size) in enumerate(stage):
        for k, source in enumerate(sources):
            for parity in (0, 1):
                def to(chip, core, c=c, start=start, size=size, k=k, parity=parity):
                    half = core if k == 0 else 1 - core
                    owner = lax.rem(chip + 2, CHIPS) * 2 + ((half if parity == 0 else 1 - half) if joined else parity)
                    return c.layer, owner * 2 + half, pl.ds(start, size)

                moves.append(Move(source, fixed(index, parity), target, to, (size, c.cols)))
    return moves


def solution(mesh):
    devices = mesh.shape["dp"]
    assert devices == 2 * CHIPS
    onward_to = [(d, (d + 2 - 4 * (d % 2)) % devices) for d in range(devices)]
    across = [(d, d ^ 1) for d in range(devices)]
    to_right = [(d, (d + 2) % devices) for d in range(devices)]
    to_left = [(d, (d - 2) % devices) for d in range(devices)]

    def halves(a, count):
        return a.reshape(a.shape[0], count, a.shape[1] // count, a.shape[2])

    def step(*arrays):
        shapes = [a.shape for a in arrays]
        terms = [halves(t[0], 2 * devices) for t in arrays[:3]]
        weights = [halves(w, 2 * devices) for w in arrays[3:6]]
        m, v = ([halves(a, 2) for a in arrays[i : i + 3]] for i in (6, 9))
        chunks, kinds, used, stages, segments = plan([w.shape for w in weights])
        results = gather_step(chunks, kinds, used, stages, segments, terms, weights, m, v)
        gathered, moments, first_stage, onward = results[:3], results[3:9], results[9:11], list(results[11:])
        late = range(len(stages) - len(chunks[-1].segments), len(stages))

        passed, crossed = {}, {}

        def hop(s, piece, to):
            passed.setdefault(s, []).append(lax.ppermute(piece, "dp", to))
            crossed.setdefault(s, []).append(lax.ppermute(passed[s][-1], "dp", across))

        hop(0, first_stage[0], to_right)
        hop(0, first_stage[1], to_left)
        onward = dict(enumerate(onward, 1))
        for s in range(1, late.start):
            hop(s, onward[s], onward_to)
        after = {s: lax.ppermute(onward[s], "dp", across) for s in late}
        whole = [None] * 3
        whole[:1] = move(known_moves(chunks, 0, 0, [(1, 2)], 0), [gathered[0], *first_stage], gathered[:1])
        sources, targets = [gathered[1], onward[1]], [gathered[1]]
        moves = known_moves(chunks, 1, 0, [None, 1], 0)
        for s in late:
            c, _, size = stages[s][0]
            for k, (piece, i) in enumerate(((onward[s], 0), (after[s], 2))):
                moves.append(Move(len(sources), fixed(i), len(targets), fixed(0, k), (size, c.cols)))
                sources.append(piece)
            targets.append(jax.ShapeDtypeStruct((1, 2, size, c.cols), BF16))
        whole[1], *joined = move(moves, sources, targets)
        for s, piece in zip(late, joined):
            hop(s, piece, onward_to)
        sources = [gathered[2], onward[2], *moments]
        moves = known_moves(chunks, 2, 0, [None, None, 1], 0)
        for a, array in enumerate(moments):
            for layer in range(array.shape[0]):
                for h in (0, 1):
                    moves.append(Move(2 + a, fixed(layer, h), 1 + a, fixed(layer, h), array.shape[2:]))
        whole[2], *moments = move(moves, sources, [gathered[2], *moments])

        whole[0] = put(first_moves(stages[0], range(4), 0), [*passed[0], *crossed[0]], whole[0])
        for place, group in enumerate(([1], [2], late), 1):
            which = stages[group[0]][0][0].which
            sources, moves = [], []
            for s in group:
                moves += last_moves(stages[s], (len(sources), len(sources) + 1), 0, joined=s in late)
                sources += [*passed[s], *crossed[s]]
            if place == 2:
                for s in late:
                    moves += late_moves(stages[s], (len(sources), len(sources) + 1), 0)
                    sources += [onward[s], after[s]]
            whole[which] = put(moves, sources, whole[which])
        return tuple(a.reshape(s) for a, s in zip((*whole, *moments), shapes[3:]))

    all_of, cut = P(None, None, None), P(None, "dp", None)
    return jax.shard_map(
        step,
        mesh=mesh,
        in_specs=(P(("rep", "dp"), None, None, None),) * 3 + (all_of,) * 3 + (cut,) * 6,
        out_specs=(P("rep", None, None),) * 3 + (P("rep", "dp", None),) * 6,
        check_vma=False,
    )
```

```python
import functools

import jax
import jax.numpy as jnp
from jax import lax
from jax.experimental import pallas as pl
from jax.experimental.pallas import tpu as pltpu
from jax.sharding import PartitionSpec as P


MESH = pl.DeviceIdType.MESH
F32, BF16 = jnp.float32, jnp.bfloat16
VMEM_LIMIT = 63 * 2**20
CHIPS = 4
OPPOSITE, RIGHT, LEFT, OWN = range(4)
OFFSET = (2, 1, 3, 0)
FIRST_ROWS = 16
LAST_ROWS = 40


def adamw(w, m, v, g):
    m = 0.9 * m + 0.1 * g
    v = 0.95 * v + 0.05 * g * g
    step = m * lax.rsqrt(v + 1e-8) + 0.1 * w
    return (w - 0.02 * step).astype(BF16), m, v


class Chunk:
    def __init__(self, number, which, layer, kind, place, rows, cols):
        self.number, self.which, self.layer = number, which, layer
        self.kind, self.place = kind, place
        self.rows, self.cols = rows, cols
        self.width = 640 if cols % 640 == 0 else 512
        self.segments = []


def plan(shapes):
    kinds, chunks, used = [], [], []
    for which, (layers, _, rows, cols) in enumerate(shapes):
        if (rows, cols) not in kinds:
            kinds.append((rows, cols))
            used.append(0)
        kind = kinds.index((rows, cols))
        for layer in range(layers):
            chunks.append(Chunk(len(chunks), which, layer, kind, used[kind], rows, cols))
            used[kind] += 1
    stages, count = [], 0
    for c in chunks:
        last = c.which == chunks[-1].which
        cuts = [0, c.rows - LAST_ROWS, c.rows] if c is chunks[-1] else [0, c.rows]
        for start, stop in zip(cuts, cuts[1:]):
            if last or not stages or stages[-1][0][0].which != c.which:
                stages.append([])
            stages[-1].append((c, start, stop - start))
            c.segments.append((count, len(stages) - 1, len(stages[-1]) - 1, start, stop - start))
            count += 1
    return chunks, kinds, used, stages, count


def exchange(chunks, kinds, used, stages, *refs):
    it = iter(refs)
    take = lambda n: [next(it) for _ in range(n)]
    g, w, m, v = take(3), take(3), take(3), take(3)
    out, new_m, new_v = take(3), take(3), take(3)
    to_go_right, to_go_left, *onward = take(len(stages) + 1)
    onward = [None, *onward]
    nk = len(kinds)
    peer, pass_in, near_in, own, w_in, m_in, v_in = (take(nk) for _ in range(7))
    (first_in, lead_sem, first_sem, lead_send, x_send, x_recv, a_send, a_recv, b_send, b_recv, own_sem, in_sem, out_sem, kept_sem, g_send, g_recv,
     gx_send, gx_recv) = it
    n = len(chunks)

    me = lax.axis_index("dp")
    chip, core = me // 2, me % 2
    right = lax.rem(chip + 1, CHIPS) * 2 + core
    left = lax.rem(chip + CHIPS - 1, CHIPS) * 2 + core
    other = chip * 2 + (1 - core)
    chip_at = [lax.rem(chip + OFFSET[r], CHIPS) for r in range(4)]
    ahead_chip, behind_chip = (lax.rem(chip + 1 + 2 * (core if s else 1 - core), CHIPS) for s in (1, 0))
    ahead, behind = ahead_chip * 2 + core, behind_chip * 2 + core

    barrier = pltpu.get_barrier_semaphore()
    for d in (chip_at[RIGHT] * 2, chip_at[LEFT] * 2, other):
        pl.semaphore_signal(barrier, inc=1, device_id={"dp": d}, device_id_type=MESH)

    def remote(src, dst, send, recv, to):
        pltpu.make_async_remote_copy(
            src_ref=src, dst_ref=dst, send_sem=send, recv_sem=recv, device_id={"dp": to}, device_id_type=MESH).start()

    def await_bytes(ref, sem):
        pltpu.make_async_copy(ref, ref, sem).wait()

    order = [(OPPOSITE, c) for c in chunks]
    for c in chunks:
        order += [(RIGHT, c), (LEFT, c)]
    order += [(OWN, c) for c in chunks]
    slots, seen = {}, [0] * nk
    for r, c in order:
        slots[r, c.number] = seen[c.kind] % 3
        seen[c.kind] += 1

    def own_load(p):
        r, c = order[p]
        slot = slots[r, c.number]
        return pltpu.make_async_copy(
            g[c.which].at[c.layer, pl.ds((chip_at[r] * 2 + core) * 2, 2)], own[c.kind].at[slot], own_sem.at[c.kind * 3 + slot])

    def load_state(c):
        s = c.place % 2
        sem = (c.kind * 2 + s) * 2
        pltpu.make_async_copy(w[c.which].at[c.layer, pl.ds(me * 2, 2)], w_in[c.kind].at[s], in_sem.at[sem]).start()
        pltpu.make_async_copy(m[c.which].at[c.layer], m_in[c.kind].at[s], in_sem.at[sem + 1]).start()
        pltpu.make_async_copy(v[c.which].at[c.layer], v_in[c.kind].at[s], in_sem.at[sem + 1]).start()

    first = chunks[0]
    pieces = [(h, rows) for rows in ((0, FIRST_ROWS), (FIRST_ROWS, first.rows)) for h in (0, 1)]

    def given(h, start, stop):
        return g[first.which].at[first.layer, (chip_at[OPPOSITE] * 2 + (1 - core)) * 2 + h, pl.ds(start, stop - start)]

    for h in (0, 1):
        pltpu.make_async_copy(given(h, 0, FIRST_ROWS), first_in.at[h], first_sem.at[0]).start()
    own_load(0).start()
    own_load(1).start()
    await_bytes(first_in, first_sem.at[0])

    @pl.when(core == 0)
    def _():
        pl.semaphore_wait(barrier, 5)

    @pl.when(core == 1)
    def _():
        pl.semaphore_wait(barrier, 1)

    def swap(r, c):
        remote(
            g[c.which].at[c.layer, pl.ds((chip_at[r] * 2 + (1 - core)) * 2, 2)], peer[c.kind].at[r, c.place],
            x_send.at[c.kind], x_recv.at[{OPPOSITE: 0, RIGHT: n, LEFT: n, OWN: 2 * n}[r] + c.number], other)

    def first_piece(h, start, stop):
        return peer[first.kind].at[OPPOSITE, first.place, h, pl.ds(start, stop - start)]

    for k, (h, (start, stop)) in enumerate(pieces):
        remote(
            first_in.at[h] if start == 0 else given(h, start, stop), first_piece(h, start, stop),
            x_send.at[first.kind], x_recv.at[3 * n + k], other)
    for c in chunks[1:]:
        swap(OPPOSITE, c)

    position = [0]

    def take_own(r, c):
        p = position[0]
        position[0] += 1
        assert order[p] == (r, c)
        if p + 2 < len(order):
            own_load(p + 2).start()
        own_load(p).wait()
        if r == RIGHT:
            await_bytes(peer[c.kind].at[pl.ds(RIGHT, 2), c.place], x_recv.at[n + c.number])
        elif r == OWN or r == OPPOSITE and c is not first:
            await_bytes(peer[c.kind].at[r, c.place], x_recv.at[(0 if r == OPPOSITE else 2 * n) + c.number])
        return own[c.kind].at[slots[r, c.number]], peer[c.kind].at[r, c.place]

    def tiles(c, start, stop, body):
        whole = (stop - start) // 16
        cols = [pl.ds(k, c.width) for k in range(0, c.cols, c.width)]

        @pl.loop(0, whole)
        def _(t):
            for k in cols:
                body(pl.ds(pl.multiple_of(start + t * 16, 16), 16), k)

        if start + whole * 16 < stop:
            for k in cols:
                body(pl.ds(start + whole * 16, stop - start - whole * 16), k)

    def add(c, h, mine, theirs, *more, rows=None):
        def tile(r, k):
            total = mine[h, r, k].astype(F32) + theirs[h, r, k].astype(F32)
            for ref in more:
                total += ref[h, r, k].astype(F32)
            theirs[h, r, k] = total.astype(BF16)

        tiles(c, *(rows or (0, c.rows)), tile)

    for c in chunks:
        mine, theirs = take_own(OPPOSITE, c)
        for k, (h, (start, stop)) in enumerate(pieces if c is first else [(0, (0, c.rows)), (1, (0, c.rows))]):
            if c is first:
                await_bytes(first_piece(h, start, stop), x_recv.at[3 * n + k])
            add(c, h, mine, theirs, rows=(start, stop))
            if c is first and k == 0:

                @pl.when(core == 1)
                def _():
                    pl.semaphore_wait(lead_sem, 1)

            remote(
                theirs.at[h, pl.ds(start, stop - start)], pass_in[c.kind].at[c.place, h, pl.ds(start, stop - start)],
                lead_send.at[0] if c is first else a_send.at[c.kind], a_recv.at[c.number], (right, left)[h])
        swap(RIGHT, c)
        swap(LEFT, c)
        if c.number == 1:

            @pl.when(core == 0)
            def _():
                await_bytes(pass_in[first.kind].at[first.place], lead_send.at[0])

        if c.number == 2:

            @pl.when(core == 0)
            def _():
                pl.semaphore_signal(lead_sem, inc=1, device_id={"dp": other}, device_id_type=MESH)

    for c in chunks:
        for r, to, side in ((RIGHT, right, 0), (LEFT, left, 1)):
            mine, theirs = take_own(r, c)
            if r == RIGHT:
                await_bytes(pass_in[c.kind].at[c.place], a_recv.at[c.number])
            for h in (side, 1 - side):
                add(c, h, mine, theirs, *([pass_in[c.kind].at[c.place]] if h == side else []))
                remote(theirs.at[h], near_in[c.kind].at[side, c.place, h], b_send.at[c.kind], b_recv.at[c.number], to)
        swap(OWN, c)

    for c in chunks[:2]:
        load_state(c)
    storing = []

    def await_moments(c):
        await_bytes(m_in[c.kind], out_sem.at[c.kind * 2 + c.place % 2])

    for c in chunks:
        mine, theirs = take_own(OWN, c)
        s = c.place % 2
        await_bytes(w_in[c.kind].at[s], in_sem.at[(c.kind * 2 + s) * 2])
        await_bytes(m_in[c.kind], in_sem.at[(c.kind * 2 + s) * 2 + 1])
        await_bytes(near_in[c.kind].at[:, c.place], b_recv.at[c.number])
        from_left, from_right = near_in[c.kind].at[0, c.place], near_in[c.kind].at[1, c.place]
        w_ref, m_ref, v_ref = w_in[c.kind].at[s], m_in[c.kind].at[s], v_in[c.kind].at[s]
        for h in (0, 1):

            def tile(r, k):
                total = mine[h, r, k].astype(F32) + theirs[h, r, k].astype(F32)
                total += from_left[h, r, k].astype(F32) + from_right[h, r, k].astype(F32)
                gradient = total.astype(BF16).astype(F32)
                new = adamw(w_ref[h, r, k].astype(F32), m_ref[h, r, k], v_ref[h, r, k], gradient)
                theirs[h, r, k], m_ref[h, r, k], v_ref[h, r, k] = new

            tiles(c, 0, c.rows, tile)
        for number, stage, index, start, size in c.segments:
            rows = pl.ds(start, size)
            here = lambda h: out[c.which].at[c.layer, me * 2 + h, rows]
            if stage == 0:
                sends = (
                    (0, right, to_go_right.at[index]), (1, right, here(1)), (1, left, to_go_left.at[index]), (0, left, here(0)))
            elif c is chunks[-1]:
                e = onward[stage]
                sends = (
                    (core, ahead, e.at[0]), (1 - core, ahead, e.at[1]), (1 - core, behind, e.at[2]), (core, behind, e.at[3]))
            else:
                sends = (
                    (core, ahead, onward[stage].at[index, core]), (1 - core, ahead, here(1 - core)),
                    (1 - core, behind, here(1 - core)), (core, behind, here(core)))
            for h, to, dst in sends:
                remote(theirs.at[h, rows], dst, g_send.at[c.kind], g_recv.at[number], to)
        target = out[c.which].at[c.layer, pl.ds(me * 2, 2)]
        remote(theirs, target, gx_send.at[c.kind], gx_recv.at[c.kind], other)
        pltpu.make_async_copy(theirs, target, kept_sem.at[c.kind]).start()
        pltpu.make_async_copy(m_ref, new_m[c.which].at[c.layer], out_sem.at[c.kind * 2 + s]).start()
        pltpu.make_async_copy(v_ref, new_v[c.which].at[c.layer], out_sem.at[c.kind * 2 + s]).start()
        storing.append(c)
        if 1 <= c.number < n - 1:
            following = chunks[c.number + 1]
            for before in storing[:-1]:
                if before.kind == following.kind and before.place == following.place - 2:
                    await_moments(before)
                    storing.remove(before)
            load_state(following)

    full = [sum(c.kind == kind for c in chunks[:-1]) for kind in range(nk)]
    for c in chunks:
        for number, stage, index, start, size in c.segments:
            rows = pl.ds(start, size)
            await_bytes(near_in[c.kind].at[:, c.place, :, rows], g_recv.at[number])
            if c is chunks[-1]:
                continue
            there = lambda owner, h: out[c.which].at[c.layer, (owner * 2 + core) * 2 + h]
            if stage == 0:
                moves = (
                    (to_go_right.at[index], there(chip_at[LEFT], 0)), (there(chip_at[LEFT], 1),) * 2,
                    (to_go_left.at[index], there(chip_at[RIGHT], 1)), (there(chip_at[RIGHT], 0),) * 2)
            else:
                mine = onward[stage].at[index, core]
                moves = (
                    (mine, there(behind_chip, core)), (there(behind_chip, 1 - core),) * 2,
                    (there(ahead_chip, 1 - core), mine), (there(ahead_chip, core),) * 2)
            for src, dst in moves:
                remote(src, dst, gx_send.at[nk + c.kind], gx_recv.at[nk + c.kind], other)
    for c in storing:
        await_moments(c)
    for kind in range(nk):
        await_bytes(peer[kind], x_send.at[kind])
        if kind == first.kind:
            await_bytes(pass_in[kind].at[pl.ds(1, used[kind] - 1)], a_send.at[kind])
        else:
            await_bytes(pass_in[kind], a_send.at[kind])
        await_bytes(peer[kind].at[pl.ds(1, 2)], b_send.at[kind])
        await_bytes(peer[kind].at[pl.ds(0, 2)], g_send.at[kind])
        await_bytes(peer[kind].at[0], gx_send.at[kind])
        await_bytes(peer[kind].at[0], gx_recv.at[kind])
        await_bytes(peer[kind].at[0], kept_sem.at[kind])
        if full[kind]:
            await_bytes(near_in[kind].at[:, pl.ds(0, full[kind])], gx_send.at[nk + kind])
            await_bytes(near_in[kind].at[:, pl.ds(0, full[kind])], gx_recv.at[nk + kind])

    @pl.when(core == 1)
    def _():
        await_bytes(pass_in[first.kind].at[first.place], lead_send.at[0])


def gather_step(chunks, kinds, used, stages, segments, terms, weights, m, v):
    n, nk = len(chunks), len(kinds)
    hbm = pl.BlockSpec(memory_space=pltpu.HBM)
    slots = lambda lead, dtype: [
        pltpu.VMEM((*(u if x is None else x for x in lead), 2, *k), dtype) for k, u in zip(kinds, used)]
    dma = lambda count: pltpu.SemaphoreType.DMA((count,))
    results = [jax.ShapeDtypeStruct(w.shape, BF16) for w in weights]
    results += [jax.ShapeDtypeStruct(a.shape, F32) for a in (*m, *v)]
    results += [jax.ShapeDtypeStruct((len(stages[0]), *kinds[stages[0][0][0].kind]), BF16)] * 2
    for s in stages[1:]:
        lead = (4,) if s[0][0] is chunks[-1] else (len(s), 2)
        results.append(jax.ShapeDtypeStruct((*lead, s[0][2], s[0][0].cols), BF16))
    return pl.pallas_call(
        functools.partial(exchange, chunks, kinds, used, stages),
        out_shape=results,
        in_specs=[hbm] * 12,
        out_specs=[hbm] * len(results),
        scratch_shapes=[
            *slots((4, None), BF16), *slots((None,), BF16), *slots((2, None), BF16), *slots((3,), BF16),
            *slots((2,), BF16), *slots((2,), F32), *slots((2,), F32),
            pltpu.VMEM((2, FIRST_ROWS, chunks[0].cols), BF16), pltpu.SemaphoreType.REGULAR, dma(1), dma(1),
            dma(nk), dma(3 * n + 4), dma(nk), dma(n), dma(nk), dma(n), dma(3 * nk), dma(4 * nk), dma(2 * nk), dma(nk),
            dma(nk), dma(segments), dma(2 * nk), dma(2 * nk),
        ],
        compiler_params=pltpu.CompilerParams(collective_id=0, has_side_effects=True, vmem_limit_bytes=VMEM_LIMIT),
    )(*terms, *weights, *m, *v)


class Move:
    def __init__(self, source, source_at, target, target_at, shape):
        self.source, self.source_at = source, source_at
        self.target, self.target_at = target, target_at
        self.shape = shape


def move_body(moves, kinds, depth, n_in, n_out, *refs):
    sources, targets = refs[:n_in], refs[n_in : n_in + n_out]
    bufs, (in_sem, out_sem) = refs[n_in + n_out : -2], refs[-2:]
    me = lax.axis_index("dp")
    chip, core = me // 2, me % 2
    seen, place = [0] * len(kinds), []
    for u in moves:
        place.append((u.kind, seen[u.kind] % depth[u.kind]))
        seen[u.kind] += 1
    sem = {slot: k for k, slot in enumerate(sorted(set(place)))}

    def load(i):
        u, (kind, slot) = moves[i], place[i]
        return pltpu.make_async_copy(
            sources[u.source].at[u.source_at(chip, core)], bufs[kind].at[slot], in_sem.at[sem[place[i]]])

    def store(i):
        u, (kind, slot) = moves[i], place[i]
        return pltpu.make_async_copy(
            bufs[kind].at[slot], targets[u.target].at[u.target_at(chip, core)], out_sem.at[sem[place[i]]])

    waited, last = set(), {}

    def start(i):
        if place[i] in last:
            store(last[place[i]]).wait()
            waited.add(last[place[i]])
        last[place[i]] = i
        load(i).start()

    ahead = 8
    for i in range(min(ahead, len(moves))):
        start(i)
    for i in range(len(moves)):
        load(i).wait()
        store(i).start()
        if i + ahead < len(moves):
            start(i + ahead)
    for i in range(len(moves)):
        if i not in waited:
            store(i).wait()


def move(moves, sources, targets):
    kinds, counts = [], []
    for u in moves:
        kind = (u.shape, sources[u.source].dtype)
        if kind not in kinds:
            kinds.append(kind)
            counts.append(0)
        u.kind = kinds.index(kind)
        counts[u.kind] += 1
    depth = [min(12, c) for c in counts]
    size = lambda shape: functools.reduce(lambda a, b: a * b, shape)
    nbytes = 2 * sum(size(shape) * dtype.itemsize * c for (shape, dtype), c in zip(kinds, counts))
    hbm = pl.BlockSpec(memory_space=pltpu.HBM)
    return pl.pallas_call(
        functools.partial(move_body, moves, kinds, depth, len(sources), len(targets)),
        out_shape=[jax.ShapeDtypeStruct(a.shape, a.dtype) for a in targets],
        in_specs=[hbm] * len(sources),
        out_specs=[hbm] * len(targets),
        scratch_shapes=[pltpu.VMEM((d, *shape), dtype) for d, (shape, dtype) in zip(depth, kinds)]
        + [pltpu.SemaphoreType.DMA((sum(depth),)), pltpu.SemaphoreType.DMA((sum(depth),))],
        compiler_params=pltpu.CompilerParams(vmem_limit_bytes=48 * 2**20),
        cost_estimate=pl.CostEstimate(flops=2 * nbytes, bytes_accessed=nbytes, transcendentals=0),
    )(*sources)


def put_body(moves, n_in, *refs):
    sources, target, sem = refs[:n_in], refs[-2], refs[-1]
    me = lax.axis_index("dp")
    chip, core = me // 2, me % 2
    copies = [
        pltpu.make_async_copy(
            sources[u.source].at[u.source_at(chip, core)], target.at[u.target_at(chip, core)], sem.at[i])
        for i, u in enumerate(moves)
    ]
    for copy in copies:
        copy.start()
    for copy in copies:
        copy.wait()


def put(moves, sources, into):
    nbytes = 2 * sum(a.size * a.dtype.itemsize for a in sources)
    hbm = pl.BlockSpec(memory_space=pltpu.HBM)
    return pl.pallas_call(
        functools.partial(put_body, moves, len(sources) + 1),
        out_shape=jax.ShapeDtypeStruct(into.shape, into.dtype),
        in_specs=[pl.BlockSpec(memory_space=pltpu.VMEM)] * len(sources) + [hbm],
        out_specs=hbm,
        input_output_aliases={len(sources): 0},
        scratch_shapes=[pltpu.SemaphoreType.DMA((len(moves),))],
        compiler_params=pltpu.CompilerParams(vmem_limit_bytes=16 * 2**20),
        cost_estimate=pl.CostEstimate(flops=2 * nbytes, bytes_accessed=nbytes, transcendentals=0),
    )(*sources, into)


def fixed(*index):
    return lambda chip, core: index


def known_moves(chunks, which, source, onward, target):
    def blocks(c, steps, block):
        return lambda chip, core: (c.layer, pl.ds((lax.rem(chip + steps * (1 + 2 * core), CHIPS) * 2 + block(core)) * 2, 2))

    def behind(c, parity, h):
        return lambda chip, core: (c.layer, (lax.rem(chip + 3 - 2 * core, CHIPS) * 2 + parity) * 2 + h(core))

    def beside(c, r, h):
        return lambda chip, core: (c.layer, (lax.rem(chip + OFFSET[r], CHIPS) * 2 + core) * 2 + h)

    def add(source, source_at, place, shape):
        moves.append(Move(source, source_at, target, place, shape))

    mine, its, moves = (lambda core: core), (lambda core: 1 - core), []
    for c in (c for c in chunks if c.which == which):
        block, piece = (2, c.rows, c.cols), (c.rows, c.cols)
        for place in (blocks(c, 0, mine), blocks(c, 0, its)):
            add(source, place, place, block)
        if c is chunks[-1]:
            continue
        ((_, stage, index, _, _),) = c.segments
        if stage == 0:
            for steps in (1, 3):
                place = blocks(c, steps, its)
                add(source, place, place, block)
            for passed, r in enumerate((LEFT, RIGHT)):
                add(onward[0][passed], fixed(index), beside(c, r, passed), piece)
                place = beside(c, r, 1 - passed)
                add(source, place, place, piece)
        else:
            for parity in (0, 1):
                place = blocks(c, 1, lambda core, parity=parity: parity)
                add(source, place, place, block)
                place = behind(c, parity, its)
                add(source, place, place, piece)
                add(onward[stage], fixed(index, parity), behind(c, parity, mine), piece)
    return moves


def late_moves(stage, sources, target):
    (c, start, size), moves = stage[0], []
    for k, source in enumerate(sources):
        for i in range(4):
            def to(chip, core, k=k, i=i):
                there = core if k == 0 else 1 - core
                owner = lax.rem(chip + (3 - 2 * there if i < 2 else 1 + 2 * there), CHIPS) * 2 + there
                return c.layer, owner * 2 + (there if i in (0, 3) else 1 - there), pl.ds(start, size)

            moves.append(Move(source, fixed(i), target, to, (size, c.cols)))
    return moves


def first_moves(stage, sources, target):
    moves = []
    for index, (c, _, _) in enumerate(stage):
        for k, source in enumerate(sources):
            def to(chip, core, c=c, k=k):
                owner = lax.rem(chip + 2, CHIPS) * 2 + (core if k < 2 else 1 - core)
                return c.layer, owner * 2 + k % 2

            moves.append(Move(source, fixed(index), target, to, (c.rows, c.cols)))
    return moves


def last_moves(stage, sources, target, joined=False):
    moves = []
    for index, (c, start, size) in enumerate(stage):
        for k, source in enumerate(sources):
            for parity in (0, 1):
                def to(chip, core, c=c, start=start, size=size, k=k, parity=parity):
                    half = core if k == 0 else 1 - core
                    owner = lax.rem(chip + 2, CHIPS) * 2 + ((half if parity == 0 else 1 - half) if joined else parity)
                    return c.layer, owner * 2 + half, pl.ds(start, size)

                moves.append(Move(source, fixed(index, parity), target, to, (size, c.cols)))
    return moves


def solution(mesh):
    devices = mesh.shape["dp"]
    assert devices == 2 * CHIPS
    onward_to = [(d, (d + 2 - 4 * (d % 2)) % devices) for d in range(devices)]
    across = [(d, d ^ 1) for d in range(devices)]
    to_right = [(d, (d + 2) % devices) for d in range(devices)]
    to_left = [(d, (d - 2) % devices) for d in range(devices)]

    def halves(a, count):
        return a.reshape(a.shape[0], count, a.shape[1] // count, a.shape[2])

    def step(*arrays):
        shapes = [a.shape for a in arrays]
        terms = [halves(t[0], 2 * devices) for t in arrays[:3]]
        weights = [halves(w, 2 * devices) for w in arrays[3:6]]
        m, v = ([halves(a, 2) for a in arrays[i : i + 3]] for i in (6, 9))
        chunks, kinds, used, stages, segments = plan([w.shape for w in weights])
        results = gather_step(chunks, kinds, used, stages, segments, terms, weights, m, v)
        gathered, moments, first_stage, onward = results[:3], results[3:9], results[9:11], list(results[11:])
        late = range(len(stages) - len(chunks[-1].segments), len(stages))

        passed, crossed = {}, {}

        def hop(s, piece, to):
            passed.setdefault(s, []).append(lax.ppermute(piece, "dp", to))
            crossed.setdefault(s, []).append(lax.ppermute(passed[s][-1], "dp", across))

        hop(0, first_stage[0], to_right)
        hop(0, first_stage[1], to_left)
        onward = dict(enumerate(onward, 1))
        for s in range(1, late.start):
            hop(s, onward[s], onward_to)
        after = {s: lax.ppermute(onward[s], "dp", across) for s in late}
        whole = [None] * 3
        whole[:1] = move(known_moves(chunks, 0, 0, [(1, 2)], 0), [gathered[0], *first_stage], gathered[:1])
        sources, targets = [gathered[1], onward[1]], [gathered[1]]
        moves = known_moves(chunks, 1, 0, [None, 1], 0)
        for s in late:
            c, _, size = stages[s][0]
            for k, (piece, i) in enumerate(((onward[s], 0), (after[s], 2))):
                moves.append(Move(len(sources), fixed(i), len(targets), fixed(0, k), (size, c.cols)))
                sources.append(piece)
            targets.append(jax.ShapeDtypeStruct((1, 2, size, c.cols), BF16))
        whole[1], *joined = move(moves, sources, targets)
        for s, piece in zip(late, joined):
            hop(s, piece, onward_to)
        sources = [gathered[2], onward[2], *moments]
        moves = known_moves(chunks, 2, 0, [None, None, 1], 0)
        for a, array in enumerate(moments):
            for layer in range(array.shape[0]):
                for h in (0, 1):
                    moves.append(Move(2 + a, fixed(layer, h), 1 + a, fixed(layer, h), array.shape[2:]))
        whole[2], *moments = move(moves, sources, [gathered[2], *moments])

        whole[0] = put(first_moves(stages[0], range(4), 0), [*passed[0], *crossed[0]], whole[0])
        for place, group in enumerate(([1], [2], late), 1):
            which = stages[group[0]][0][0].which
            sources, moves = [], []
            for s in group:
                moves += last_moves(stages[s], (len(sources), len(sources) + 1), 0, joined=s in late)
                sources += [*passed[s], *crossed[s]]
            if place == 2:
                for s in late:
                    moves += late_moves(stages[s], (len(sources), len(sources) + 1), 0)
                    sources += [onward[s], after[s]]
            whole[which] = put(moves, sources, whole[which])
        return tuple(a.reshape(s) for a, s in zip((*whole, *moments), shapes[3:]))

    all_of, cut = P(None, None, None), P(None, "dp", None)
    return jax.shard_map(
        step,
        mesh=mesh,
        in_specs=(P(("rep", "dp"), None, None, None),) * 3 + (all_of,) * 3 + (cut,) * 6,
        out_specs=(P("rep", None, None),) * 3 + (P("rep", "dp", None),) * 6,
        check_vma=False,
    )
```
